128 devices in a mesh: gx: 4 (over x), gy: 32 (over y, z, core).
Axes of the slice: x: 4, y: 4, z: 4, core: 2. Of those that a mesh axis runs over, the one named last changes fastest.
Arguments:
- grid_latent: bfloat16 [65536, 512], P(('gx', 'gy')), may hold values from -6 to 6
- mesh_latent: bfloat16 [16384, 512], P(('gx', 'gy')), may hold values from -6 to 6
- encode_senders: int32 [32, 16384], P(None, ('gx', 'gy')), may hold values from -1 to 65535, as said below
- mesh_senders: int32 [32, 16384], P(None, ('gx', 'gy')), may hold values from -1 to 16383, as said below
- decode_senders: int32 [3, 65536], P(None, ('gx', 'gy')), may hold values from 0 to 16383, as said below
- encoder_edges: bfloat16 [3, 512, 512], replicated, may hold values from -0.25 to 0.25
- encoder_edgebias: float32 [2, 512], replicated, may hold values from -3 to 3
- encoder_nodes: bfloat16 [3, 512, 512], replicated, may hold values from -0.25 to 0.25
- encoder_nodebias: float32 [2, 512], replicated, may hold values from -3 to 3
- process_edges: bfloat16 [3, 512, 512], replicated, may hold values from -0.25 to 0.25
- process_edgebias: float32 [2, 512], replicated, may hold values from -3 to 3
- process_nodes: bfloat16 [3, 512, 512], replicated, may hold values from -0.25 to 0.25
- process_nodebias: float32 [2, 512], replicated, may hold values from -3 to 3
- decoder_edges: bfloat16 [3, 512, 512], replicated, may hold values from -0.25 to 0.25
- decoder_edgebias: float32 [2, 512], replicated, may hold values from -3 to 3
- decoder_nodes: bfloat16 [3, 512, 512], replicated, may hold values from -0.25 to 0.25
- decoder_nodebias: float32 [2, 512], replicated, may hold values from -3 to 3
Outputs:
- decoded_grid: bfloat16 [65536, 512], P(('gx', 'gy'))
- processed_mesh: bfloat16 [16384, 512], P(('gx', 'gy'))
The draws below stay inside these ranges and needn't reach their ends.
Inputs may be any that keep to these rules, and one draw needn't show every extreme that they name: `encode_senders`: devices form a torus of regions, device number = gx index * gy size + gy index, and device d owns grid points d * 512 to (d + 1) * 512 - 1. In each column the live senders come first, then -1; a column has 8 to 32 live senders and some column has 32. A live sender is a grid point of the column's own device, or one of the first 128 grid points of one of the eight devices around it on the torus (wrapping on both axes). `mesh_senders`: device d owns mesh nodes d * 128 to (d + 1) * 128 - 1. In each column the live senders come first, then -1; a column has 8 to 32 live senders and some column has 32. A live sender is a mesh node of the column's own device, or one of the first 32 mesh nodes of one of the eight devices around it on the torus, or one of the first 4 mesh nodes of any device. `decode_senders`: every entry is live: a mesh node of the grid point's own device, or one of the first 32 mesh nodes of one of the eight devices around it on the torus.
All inputs are finite; a program needn't handle non-finite values.
Results may differ from the reference program's by a relative error of at most 0.013.
Values may be sent and summed in bfloat16 or wider, within the bound.
A program may use at most 64 MiB of HBM per device.

```python
import jax
import jax.numpy as jnp
from jax import lax

D = 512
G_DEV = 512
M_DEV = 128
K1 = 32
KM = 32
K3 = 3
CM = 4
GRID = 65536
MESH = 16384
N_GX = 4
N_GY = 32


def sender_table(key, degree, receivers, senders, border, coarse, own_share, far_share, least):
    devices = N_GX * N_GY
    total = receivers * devices
    keys = jax.random.split(key, 7)
    column = jnp.arange(total, dtype=jnp.int32)
    device = column // receivers
    place_x = device // N_GY
    place_y = device % N_GY
    kind = jax.random.randint(keys[0], (degree, total), 0, 100)
    which = jax.random.randint(keys[1], (degree, total), 0, 8)
    table_x = jnp.array([-1, -1, -1, 0, 0, 1, 1, 1], jnp.int32)
    table_y = jnp.array([-1, 0, 1, -1, 1, -1, 0, 1], jnp.int32)
    near_x = (place_x[None] + table_x[which]) % N_GX
    near_y = (place_y[None] + table_y[which]) % N_GY
    near_device = near_x * N_GY + near_y
    far_device = jax.random.randint(keys[2], (degree, total), 0, devices)
    own_row = jax.random.randint(keys[3], (degree, total), 0, senders)
    near_row = jax.random.randint(keys[4], (degree, total), 0, border)
    far_row = jax.random.randint(keys[5], (degree, total), 0, max(coarse, 1))
    is_own = kind < own_share
    is_far = kind >= 100 - far_share
    source = jnp.where(is_own, device[None], jnp.where(is_far, far_device, near_device))
    offset = jnp.where(is_own, own_row, jnp.where(is_far, far_row, near_row))
    sender_ids = (source * senders + offset).astype(jnp.int32)
    polar = (place_x == 0) | (place_x == N_GX - 1)
    split = least + (degree - least) * 3 // 4
    lower = jnp.where(polar, split, least)
    upper = jnp.where(polar, degree + 1, split + 1)
    counts = jax.random.randint(keys[6], (total,), lower, upper)
    leading = column % receivers == 0
    counts = jnp.where(leading & polar, degree, counts)
    slots = jnp.arange(degree, dtype=jnp.int32)[:, None]
    return jnp.where(slots < counts[None], sender_ids, -1).astype(jnp.int32)


def draw_encode_senders(key, part):
    return sender_table(jax.random.fold_in(key, 11), K1, M_DEV, G_DEV, G_DEV // 4, 0, 50, 0, K1 // 4)


def draw_mesh_senders(key, part):
    return sender_table(jax.random.fold_in(key, 23), KM, M_DEV, M_DEV, M_DEV // 4, CM, 40, 30, KM // 4)


def draw_decode_senders(key, part):
    return sender_table(jax.random.fold_in(key, 37), K3, G_DEV, M_DEV, M_DEV // 4, 0, 50, 0, K3)


def block_scale(own_key, extent, cuts, low, high):
    factor_of = 1.0
    for dim, blocks in cuts:
        draws = jax.random.uniform(jax.random.fold_in(jax.random.fold_in(own_key, 6), dim), (blocks,), jnp.float32, low / len(cuts), high / len(cuts))
        factor_of = factor_of * jnp.repeat(jnp.exp(draws), extent[dim] // blocks).reshape((-1,) + (1,) * (len(extent) - 1 - dim))
    return factor_of


def noise(key, shape, scale, limit, shards=(), kind=jnp.bfloat16):
    result = jax.random.normal(key, shape, jnp.float32) * scale
    if len(shards) > 0:
        result = block_scale(key, shape, shards, -0.22, 0.18) * result
    return jnp.clip(result, min=-limit, max=limit).astype(kind)


def setup_inputs(seed: int = 0) -> dict:
    arg_keys = jax.random.split(jax.random.key(seed), 18)
    return {
        "grid_latent": noise(arg_keys[0], (GRID, D), 1.0, 6.0, ((0, 128),)),
        "mesh_latent": noise(arg_keys[1], (MESH, D), 1.0, 6.0, ((0, 128),)),
        "encode_senders": draw_encode_senders(jax.random.fold_in(arg_keys[17], 71), 0),
        "mesh_senders": draw_mesh_senders(jax.random.fold_in(arg_keys[17], 71), 0),
        "decode_senders": draw_decode_senders(jax.random.fold_in(arg_keys[17], 71), 0),
        "encoder_edges": noise(arg_keys[5], (3, D, D), D ** -0.5, 0.25),
        "encoder_edgebias": noise(arg_keys[6], (2, D), 0.3, 3.0, (), jnp.float32),
        "encoder_nodes": noise(arg_keys[7], (3, D, D), D ** -0.5, 0.25),
        "encoder_nodebias": noise(arg_keys[8], (2, D), 0.3, 3.0, (), jnp.float32),
        "process_edges": noise(arg_keys[9], (3, D, D), D ** -0.5, 0.25),
        "process_edgebias": noise(arg_keys[10], (2, D), 0.3, 3.0, (), jnp.float32),
        "process_nodes": noise(arg_keys[11], (3, D, D), D ** -0.5, 0.25),
        "process_nodebias": noise(arg_keys[12], (2, D), 0.3, 3.0, (), jnp.float32),
        "decoder_edges": noise(arg_keys[13], (3, D, D), D ** -0.5, 0.25),
        "decoder_edgebias": noise(arg_keys[14], (2, D), 0.3, 3.0, (), jnp.float32),
        "decoder_nodes": noise(arg_keys[15], (3, D, D), D ** -0.5, 0.25),
        "decoder_nodebias": noise(arg_keys[16], (2, D), 0.3, 3.0, (), jnp.float32),
    }


def project(latent, weight):
    return jnp.dot(latent, weight, preferred_element_type=jnp.float32)

def finish(preact, weights, vectors):
    hidden = jax.nn.silu(preact).astype(jnp.bfloat16)
    output = jnp.dot(hidden, weights[2], preferred_element_type=jnp.float32)
    centre = lax.optimization_barrier(jnp.mean(output, axis=-1, keepdims=True))
    centred = output - centre
    spread = lax.optimization_barrier(jnp.mean(centred * centred, axis=-1, keepdims=True))
    return centred * lax.rsqrt(spread + 1e-05) * (1.0 + vectors[1])

def block_size(count, degree):
    target = max(1, 4096 // degree)
    chosen = min(count, target)
    while count % chosen:
        chosen -= 1
    return chosen

def aggregate(table, receiving, positions, active, weights, vectors):
    degree, count = positions.shape
    chosen = block_size(count, degree)
    blocks = count // chosen
    width = table.shape[1]
    shifted = (receiving + vectors[0]).reshape(blocks, chosen, width)
    places = positions.reshape(degree, blocks, chosen).transpose(1, 0, 2)
    masks = active.reshape(degree, blocks, chosen).transpose(1, 0, 2)

    def one_block(item):
        base, place, present = item
        gathered = jnp.take(table, place, axis=0)
        preact = gathered + base[None]
        message = finish(preact.reshape(degree * chosen, width), weights, vectors)
        message = message.reshape(degree, chosen, width)
        return lax.optimization_barrier(jnp.sum(jnp.where(present[..., None], message, 0.0), axis=0))
    return lax.map(one_block, (shifted, places, masks)).reshape(count, width)

def update(latent, summed, weights, vectors):
    preact = project(latent, weights[0]) + project(summed.astype(jnp.bfloat16), weights[1]) + vectors[0]
    return (latent.astype(jnp.float32) + finish(preact, weights, vectors)).astype(jnp.bfloat16)

def edge_sums(sender_latent, receiver_latent, senders, weights, vectors):
    table = project(sender_latent, weights[0])
    receiving = project(receiver_latent, weights[1])
    return aggregate(table, receiving, jnp.maximum(senders, 0).astype(jnp.int32), senders >= 0, weights, vectors)

def reference(grid_latent, mesh_latent, encode_senders, mesh_senders, decode_senders, encoder_edges, encoder_edgebias, encoder_nodes, encoder_nodebias, process_edges, process_edgebias, process_nodes, process_nodebias, decoder_edges, decoder_edgebias, decoder_nodes, decoder_nodebias):
    summed = edge_sums(grid_latent, mesh_latent, encode_senders, encoder_edges, encoder_edgebias)
    encoded = update(mesh_latent, summed, encoder_nodes, encoder_nodebias)
    summed = edge_sums(encoded, encoded, mesh_senders, process_edges, process_edgebias)
    processed = update(encoded, summed, process_nodes, process_nodebias)
    summed = edge_sums(processed, grid_latent, decode_senders, decoder_edges, decoder_edgebias)
    decoded = update(grid_latent, summed, decoder_nodes, decoder_nodebias)
    return (decoded, processed)
```

```python
import functools

import jax
import jax.numpy as jnp
from jax import lax
from jax.experimental import pallas as pl
from jax.experimental.pallas import tpu as pltpu
from jax.sharding import PartitionSpec as P

MESH = pl.DeviceIdType.MESH
F32 = jnp.float32
BF16 = jnp.bfloat16

D = 512
G = 512
M = 128
K = 32
K3 = 3
CM = 4
GB = G // 4
MB = M // 4
NX = 4
NY = 32
CHIPS = NX * NY // 2

DEAD = 1
OWN = 2
RIM1 = OWN + G
ROWS1 = RIM1 + 9 * GB
RIM2 = OWN + M
COARSE = RIM2 + 9 * MB
ROWS2 = COARSE + 2 * CHIPS * CM
ROWS3 = COARSE

R = 16
BLOCKS = M // R
E = R * K
R3 = 128
BLOCKS3 = G // R3
E3 = R3 * K3


def log2(n):
    bits = n.bit_length() - 1
    assert n == 1 << bits
    return bits


def rows_of(ids, rows, border, rim, px, py):
    owner = lax.shift_right_arithmetic(ids, log2(rows))
    off = ids & (rows - 1)
    ox = lax.shift_right_arithmetic(owner, log2(NY))
    oy = owner & (NY - 1)
    dx = (ox - px) & (NX - 1)
    dy = (oy - py) & (NY - 1)
    sx = jnp.where(dx == 1, 2, jnp.where(dx == NX - 1, 0, 1))
    sy = jnp.where(dy == 1, 2, jnp.where(dy == NY - 1, 0, 1))
    near = ((dx <= 1) | (dx == NX - 1)) & ((dy <= 1) | (dy == NY - 1)) & (off < border)
    itself = (dx == 0) & (dy == 0)
    place = (owner & 1) * CHIPS + lax.shift_right_arithmetic(owner, 1)
    far = COARSE + place * CM + (off & (CM - 1))
    row = jnp.where(near, rim + (sx * 3 + sy) * border + off, far)
    row = jnp.where(itself, OWN + off, row)
    return jnp.where(ids < 0, DEAD, row)


def silu_half(y):
    return y * jnp.tanh(y) + y


def kernel(
    grid, mesh, encs, mshs, decs, w0, v0, w1, v1, w2, v2, w3, v3, w4, v4, w5, v5,
    out_grid, out_mesh,
    grid_v, mesh_v, encs_v, mshs_v, decs_v, w_v, v_v,
    pos1, pos2, pos3, idx_a, idx_b,
    tab1, tab2, tab3, base, nodebase, base3, nodebase3,
    gat_a, gat_b, hid_a, hid_b, mlp_a, mlp_b,
    aggb, enc_v, prc_v, dec_v, aggb3, hidn,
    send1, rim1, send2, rim2, coarse, send3, rim3,
    in_sem, w_sem, idx_sem, out_sem,
    s1_sem, r1_sem, s2_sem, r2_sem, s3_sem, r3_sem, sc_sem, rc_sem, sf_sem, rf_sem,
):
    px = lax.axis_index("gx")
    py = lax.axis_index("gy")
    core = py & 1
    chip = px * (NY // 2) + lax.shift_right_logical(py, 1)

    small = [
        (grid, grid_v), (mesh, mesh_v), (encs, encs_v), (mshs, mshs_v), (decs, decs_v),
        (v0, v_v.at[0]), (v1, v_v.at[1]), (v2, v_v.at[2]),
        (v3, v_v.at[3]), (v4, v_v.at[4]), (v5, v_v.at[5]),
    ]
    loads = [pltpu.make_async_copy(s, d, in_sem.at[i]) for i, (s, d) in enumerate(small)]
    wloads = [
        pltpu.make_async_copy(s, w_v.at[i], w_sem.at[i])
        for i, s in enumerate((w0, w1, w2, w3, w4, w5))
    ]
    loads[0].start()
    wloads[0].start()
    for c in loads[1:]:
        c.start()
    for i in (4, 5, 1, 2, 3):
        wloads[i].start()

    def at(dx, dy):
        return ((px + dx) & (NX - 1), (py + dy) & (NY - 1))

    def spread(buf, off, rows, value):
        for c in range(4):
            buf[pl.ds(off * 4 + c, rows, stride=4), :] = value[:, 128 * c : 128 * c + 128]

    def halo(src, rim, s_sem, r_sem, steps):
        copies = []
        for dx, dy in steps:
            slot = (1 - dx) * 3 + (1 - dy)
            copies.append(
                pltpu.make_async_remote_copy(
                    src_ref=src, dst_ref=rim.at[slot], send_sem=s_sem.at[slot],
                    recv_sem=r_sem.at[slot], device_id=at(dx, dy), device_id_type=MESH,
                )
            )
        for c in copies:
            c.start()
        return copies

    loads[0].wait()
    wloads[0].wait()
    own = jnp.dot(grid_v[0:GB, :], w_v[0, 0], preferred_element_type=F32) * 0.5
    spread(tab1, OWN, GB, own)
    send1[...] = tab1[OWN * 4 : (OWN + GB) * 4, :].astype(BF16)
    first = halo(send1, rim1, s1_sem, r1_sem, ((1, 0), (-1, 0), (0, 1), (0, -1)))

    for c in loads[1:]:
        c.wait()
    own = jnp.dot(grid_v[GB:G, :], w_v[0, 0], preferred_element_type=F32) * 0.5
    spread(tab1, OWN + GB, G - GB, own)
    dead = jnp.full((8, 128), -1e30, F32)
    for t in (tab1, tab2, tab3):
        t[0:8, :] = dead
    for t, rows in ((tab1, ROWS1), (tab2, ROWS2), (tab3, ROWS3)):
        t[rows * 4 : rows * 4 + 8, :] = dead

    lane = lax.broadcasted_iota(jnp.int32, (M, K), 0)
    odd = (lane & 1) * 4
    for src, pos, rows, border, rim in ((encs_v, pos1, G, GB, RIM1), (mshs_v, pos2, M, MB, RIM2)):
        row = rows_of(src[...], rows, border, rim, px, py)
        pos[0:M, :] = jnp.zeros((M, 128), jnp.int32)
        pos[M : M + 2 * R, :] = jnp.zeros((2 * R, 128), jnp.int32)
        pos[0:M, 0:K] = row.T * 4 - odd
    odd3 = (lax.broadcasted_iota(jnp.int32, (K3, R3), 1) & 1) * 4
    pos3[...] = jnp.zeros(pos3.shape, jnp.int32)
    for b in range(BLOCKS3):
        row = rows_of(decs_v[:, R3 * b : R3 * b + R3], M, MB, RIM2, px, py)
        pos3[b, 0:K3, :] = row * 4 - odd3

    def centre(i):
        def some(j, carry):
            at_rows = pl.ds(pl.multiple_of(j * 64, 64), 64)
            w = w_v[i, 2, at_rows, :].astype(F32)
            w_v[i, 2, at_rows, :] = (w - jnp.mean(w, axis=1, keepdims=True)).astype(BF16)
            return carry

        lax.fori_loop(0, D // 64, some, 0)

    def bias(i):
        return v_v[i, 0:1, :]

    def gain(i):
        return 1.0 + v_v[i, 1:2, :]

    def dot(a, b):
        return jnp.dot(a, b, preferred_element_type=F32)

    base[...] = (dot(mesh_v[...], w_v[0, 1]) + bias(0)) * 0.5
    centre(0)
    for i in (4, 5, 1, 2, 3):
        wloads[i].wait()
        centre(i)
    nodebase[...] = dot(mesh_v[...], w_v[1, 0]) + bias(1)
    base3[...] = (dot(grid_v[...], w_v[4, 1]) + bias(4)) * 0.5
    nodebase3[...] = dot(grid_v[...], w_v[5, 0]) + bias(5)

    first[0].wait_recv()
    first[1].wait_recv()
    second = []
    for sx in (0, 2):
        for dy in (1, -1):
            slot = sx * 3 + 1 - dy
            second.append(
                pltpu.make_async_remote_copy(
                    src_ref=rim1.at[sx * 3 + 1], dst_ref=rim1.at[slot], send_sem=s1_sem.at[slot],
                    recv_sem=r1_sem.at[slot], device_id=at(0, dy), device_id_type=MESH,
                )
            )
    for c in second:
        c.start()
    for c in first[2:] + second:
        c.wait_recv()
    for slot in (0, 1, 2, 3, 5, 6, 7, 8):
        lo = (RIM1 + slot * GB) * 4
        tab1[lo : lo + GB * 4, :] = rim1[slot].astype(F32)
    for c in first + second:
        c.wait_send()

    def update(i, rows, x, agg, node, new):
        n = rows.size
        p = node[rows, :] + dot(agg[rows, :], w_v[i, 1])
        o = dot(silu_half(p * 0.5).astype(BF16), w_v[i, 2])
        s = lax.rsqrt(jnp.mean(o * o, axis=1, keepdims=True) + 1e-5)
        new[rows, :] = (x[rows, :].astype(F32) + o * s * gain(i)).astype(BF16)

    def gather(tab, idx, gat, slots, receivers, by_row):
        low = lax.broadcasted_iota(jnp.int32, (8, 128), 0) < 4
        for k in range(slots):
            for r in range(0, receivers, 2):
                ia = idx[r, k] if by_row else idx[k, r]
                ib = idx[r + 1, k] if by_row else idx[k, r + 1]
                e = k * receivers + r
                gat[4 * e : 4 * e + 8, :] = jnp.where(low, tab[pl.ds(ia, 8), :], tab[pl.ds(ib, 8), :])

    def messages(i, gat, hid, mlp, slots, receivers, base_ref, base_row, agg):
        for c in range(4):
            cols = slice(128 * c, 128 * c + 128)
            for r in range(0, receivers, 16):
                b = base_ref[pl.ds(base_row + r, 16), cols]
                for k in range(slots):
                    e = k * receivers + r
                    y = gat[pl.ds(4 * e + c, 16, stride=4), :] + b
                    hid[e : e + 16, cols] = silu_half(y).astype(BF16)
        edges = slots * receivers
        mlp[0:edges, :] = dot(hid[0:edges, :], w_v[i, 2])
        g = gain(i)
        for r in range(0, receivers, 16):
            total = jnp.zeros((16, D), F32)
            for k in range(slots):
                e = k * receivers + r
                o = mlp[e : e + 16, :]
                total += o * lax.rsqrt(jnp.mean(o * o, axis=1, keepdims=True) + 1e-5)
            agg[pl.ds(base_row + r, 16), :] = (total * g).astype(BF16)

    def mesh_step(i, tab, pos, after_first):
        def fetch(b, idx, sem):
            return pltpu.make_async_copy(pos.at[pl.ds(pl.multiple_of(b * R, R), R), :], idx, sem)

        fetch(0, idx_a, idx_sem.at[0]).start()
        fetch(1, idx_b, idx_sem.at[1]).start()
        fetch(0, idx_a, idx_sem.at[0]).wait()
        gather(tab, idx_a, gat_a, K, R, True)

        def two(j, carry):
            fetch(2 * j + 2, idx_a, idx_sem.at[0]).start()
            fetch(2 * j + 1, idx_b, idx_sem.at[1]).wait()
            gather(tab, idx_b, gat_b, K, R, True)
            row = pl.multiple_of(j * (2 * R), 2 * R)
            messages(i, gat_a, hid_a, mlp_a, K, R, base, row, aggb)
            fetch(2 * j + 2, idx_a, idx_sem.at[0]).wait()
            fetch(2 * j + 3, idx_b, idx_sem.at[1]).start()
            gather(tab, idx_a, gat_a, K, R, True)
            messages(i, gat_b, hid_b, mlp_b, K, R, base, row + R, aggb)
            pl.when(j == 0)(after_first)
            return carry

        lax.fori_loop(0, BLOCKS // 2, two, 0)
        fetch(1, idx_b, idx_sem.at[1]).wait()

    ring = ((1, 0), (-1, 0), (0, 1), (0, -1), (1, 1), (1, -1), (-1, 1), (-1, -1))
    head = pl.ds(0, MB)
    tail = pl.ds(MB, M - MB)

    def halo_copies(src, rim, s_sem, r_sem):
        return [
            pltpu.make_async_remote_copy(
                src_ref=src, dst_ref=rim.at[(1 - dx) * 3 + 1 - dy],
                send_sem=s_sem.at[(1 - dx) * 3 + 1 - dy], recv_sem=r_sem.at[(1 - dx) * 3 + 1 - dy],
                device_id=at(dx, dy), device_id_type=MESH,
            )
            for dx, dy in ring
        ]

    coarse[core, chip] = jnp.zeros((4 * CM, 128), BF16)

    def coarse_copy(j):
        to = (chip + j) & (CHIPS - 1)
        return pltpu.make_async_remote_copy(
            src_ref=send2.at[0 : 4 * CM], dst_ref=coarse.at[core, chip], send_sem=sc_sem, recv_sem=rc_sem,
            device_id=(lax.shift_right_logical(to, log2(NY // 2)), (to & (NY // 2 - 1)) * 2 + core),
            device_id_type=MESH,
        )

    def coarse_all():
        return pltpu.make_async_remote_copy(
            src_ref=coarse.at[core, 0 : CHIPS - 1], dst_ref=coarse.at[core, 0 : CHIPS - 1],
            send_sem=sc_sem, recv_sem=rc_sem, device_id=at(0, 1), device_id_type=MESH,
        )

    def send_encoded():
        update(1, head, mesh_v, aggb, nodebase, enc_v)
        spread(tab2, OWN, MB, dot(enc_v[head, :], w_v[2, 0]) * 0.5)
        send2[...] = tab2[OWN * 4 : (OWN + MB) * 4, :].astype(BF16)

        def one(j, carry):
            coarse_copy(j).start()
            return carry

        lax.fori_loop(1, CHIPS, one, 0)
        for c in halo_copies(send2, rim2, s2_sem, r2_sem):
            c.start()

    mesh_step(0, tab1, pos1, send_encoded)
    update(1, tail, mesh_v, aggb, nodebase, enc_v)

    coarse_all().wait_recv()
    forward = pltpu.make_async_remote_copy(
        src_ref=coarse.at[core], dst_ref=coarse.at[core], send_sem=sf_sem, recv_sem=rf_sem,
        device_id=(px, py ^ 1), device_id_type=MESH,
    )
    forward.start()
    spread(tab2, OWN, M, dot(enc_v[...], w_v[2, 0]) * 0.5)
    base[...] = (dot(enc_v[...], w_v[2, 1]) + bias(2)) * 0.5
    nodebase[...] = dot(enc_v[...], w_v[3, 0]) + bias(3)
    copies = halo_copies(send2, rim2, s2_sem, r2_sem)
    for c in copies:
        c.wait_recv()
    for slot in (0, 1, 2, 3, 5, 6, 7, 8):
        lo = (RIM2 + slot * MB) * 4
        tab2[lo : lo + MB * 4, :] = rim2[slot].astype(F32)
    forward.wait_recv()
    for a in range(2):
        lo = (COARSE + a * CHIPS * CM) * 4
        tab2[lo : lo + CHIPS * CM * 4, :] = coarse[a].reshape(CHIPS * CM * 4, 128).astype(F32)
    for c in copies:
        c.wait_send()
    coarse_all().wait_send()
    forward.wait_send()

    def send_processed():
        update(3, head, enc_v, aggb, nodebase, prc_v)
        spread(tab3, OWN, MB, dot(prc_v[head, :], w_v[4, 0]) * 0.5)
        send3[...] = tab3[OWN * 4 : (OWN + MB) * 4, :].astype(BF16)
        for c in halo_copies(send3, rim3, s3_sem, r3_sem):
            c.start()

    mesh_step(2, tab2, pos2, send_processed)
    update(3, tail, enc_v, aggb, nodebase, prc_v)
    put_mesh = pltpu.make_async_copy(prc_v, out_mesh, out_sem.at[0])
    put_mesh.start()

    spread(tab3, OWN, M, dot(prc_v[...], w_v[4, 0]) * 0.5)
    copies = halo_copies(send3, rim3, s3_sem, r3_sem)
    for c in copies:
        c.wait_recv()
    for slot in (0, 1, 2, 3, 5, 6, 7, 8):
        lo = (RIM2 + slot * MB) * 4
        tab3[lo : lo + MB * 4, :] = rim3[slot].astype(F32)
    for c in copies:
        c.wait_send()

    def fetch3(b):
        return pltpu.make_async_copy(pos3.at[b], idx_a.at[0:8, :], idx_sem.at[0])

    def one3(b, carry):
        fetch3(b).start()
        fetch3(b).wait()
        gather(tab3, idx_a, gat_a, K3, R3, False)
        messages(4, gat_a, hid_a, mlp_a, K3, R3, base3, pl.multiple_of(b * R3, R3), aggb3)
        return carry

    lax.fori_loop(0, BLOCKS3, one3, 0)
    update(5, pl.ds(0, G), grid_v, aggb3, nodebase3, dec_v)
    put_grid = pltpu.make_async_copy(dec_v, out_grid, out_sem.at[1])
    put_grid.start()
    put_mesh.wait()
    put_grid.wait()


def per_device(*args):
    any_space = pl.BlockSpec(memory_space=pl.ANY)
    dma = pltpu.SemaphoreType.DMA
    vm = pltpu.VMEM
    i32 = jnp.int32
    return pl.pallas_call(
        kernel,
        out_shape=(jax.ShapeDtypeStruct((G, D), BF16), jax.ShapeDtypeStruct((M, D), BF16)),
        in_specs=[any_space] * len(args),
        out_specs=(any_space, any_space),
        scratch_shapes=[
            vm((G, D), BF16), vm((M, D), BF16), vm((K, M), i32), vm((K, M), i32), vm((K3, G), i32),
            vm((6, 3, D, D), BF16), vm((6, 2, D), F32),
            vm((M + 2 * R, 128), i32), vm((M + 2 * R, 128), i32), vm((BLOCKS3, 8, 128), i32),
            pltpu.SMEM((R, 128), i32), pltpu.SMEM((R, 128), i32),
            vm((ROWS1 * 4 + 8, 128), F32), vm((ROWS2 * 4 + 8, 128), F32), vm((ROWS3 * 4 + 8, 128), F32),
            vm((M, D), F32), vm((M, D), F32), vm((G, D), F32), vm((G, D), F32),
            vm((E * 4, 128), F32), vm((E * 4, 128), F32),
            vm((E, D), BF16), vm((E, D), BF16), vm((E, D), F32), vm((E, D), F32),
            vm((M, D), BF16), vm((M, D), BF16), vm((M, D), BF16), vm((G, D), BF16), vm((G, D), BF16), vm((M, D), BF16),
            vm((GB * 4, 128), BF16), vm((9, GB * 4, 128), BF16),
            vm((MB * 4, 128), BF16), vm((9, MB * 4, 128), BF16),
            vm((2, CHIPS, CM * 4, 128), BF16),
            vm((MB * 4, 128), BF16), vm((9, MB * 4, 128), BF16),
            dma((11,)), dma((6,)), dma((2,)), dma((2,)),
            dma((9,)), dma((9,)), dma((9,)), dma((9,)), dma((9,)), dma((9,)),
            dma, dma, dma, dma,
        ],
        compiler_params=pltpu.CompilerParams(has_side_effects=True, vmem_limit_bytes=60 * 1024 * 1024),
    )(*args)


def solution(mesh):
    assert dict(mesh.shape) == {"gx": NX, "gy": NY}
    split = P(("gx", "gy"), None)
    lists = P(None, ("gx", "gy"))
    return jax.shard_map(
        per_device,
        mesh=mesh,
        in_specs=(split, split, lists, lists, lists) + (P(),) * 12,
        out_specs=(split, split),
        check_vma=False,
    )
```

```python
import functools

import jax
import jax.numpy as jnp
from jax import lax
from jax.experimental import pallas as pl
from jax.experimental.pallas import tpu as pltpu
from jax.sharding import PartitionSpec as P

MESH = pl.DeviceIdType.MESH
F32 = jnp.float32
BF16 = jnp.bfloat16

D = 512
G = 512
M = 128
K = 32
K3 = 3
CM = 4
GB = G // 4
MB = M // 4
NX = 4
NY = 32
CHIPS = NX * NY // 2

DEAD = 1
OWN = 2
RIM1 = OWN + G
ROWS1 = RIM1 + 9 * GB
RIM2 = OWN + M
COARSE = RIM2 + 9 * MB
ROWS2 = COARSE + 2 * CHIPS * CM
ROWS3 = COARSE

R = 16
BLOCKS = M // R
E = R * K
R3 = 128
BLOCKS3 = G // R3
E3 = R3 * K3
HALF = GB * 2


def log2(n):
    bits = n.bit_length() - 1
    assert n == 1 << bits
    return bits


def rows_of(ids, rows, border, rim, px, py):
    owner = lax.shift_right_arithmetic(ids, log2(rows))
    off = ids & (rows - 1)
    ox = lax.shift_right_arithmetic(owner, log2(NY))
    oy = owner & (NY - 1)
    dx = (ox - px) & (NX - 1)
    dy = (oy - py) & (NY - 1)
    sx = jnp.where(dx == 1, 2, jnp.where(dx == NX - 1, 0, 1))
    sy = jnp.where(dy == 1, 2, jnp.where(dy == NY - 1, 0, 1))
    near = ((dx <= 1) | (dx == NX - 1)) & ((dy <= 1) | (dy == NY - 1)) & (off < border)
    itself = (dx == 0) & (dy == 0)
    place = (owner & 1) * CHIPS + lax.shift_right_arithmetic(owner, 1)
    far = COARSE + place * CM + (off & (CM - 1))
    row = jnp.where(near, rim + (sx * 3 + sy) * border + off, far)
    row = jnp.where(itself, OWN + off, row)
    return jnp.where(ids < 0, DEAD, row)


def silu_half(y):
    return y * jnp.tanh(y) + y


def kernel(
    grid, mesh, encs, mshs, decs, w0, v0, w1, v1, w2, v2, w3, v3, w4, v4, w5, v5,
    out_grid, out_mesh,
    grid_v, mesh_v, encs_v, mshs_v, decs_v, w_v, v_v,
    pos1, pos2, pos3, idx1, idx2, idx3,
    tab1, tab2, tab3, base, nodebase, base3, nodebase3,
    gat_a, gat_b, hid_a, hid_b, mlp_a, mlp_b,
    aggb, enc_v, prc_v, dec_v, aggb3,
    send1, rim1, send2, rim2, coarse, send3, rim3,
    in_sem, w_sem, idx_sem, out_sem,
    s1_sem, r1_sem, s2_sem, r2_sem, s3_sem, r3_sem, sc_sem, rc_sem, sf_sem, rf_sem,
    meet_a, meet_b,
):
    px = lax.axis_index("gx")
    py = lax.axis_index("gy")
    core = py & 1
    chip = px * (NY // 2) + lax.shift_right_logical(py, 1)

    def at(dx, dy):
        return ((px + dx) & (NX - 1), (py + dy) & (NY - 1))

    ring = ((1, 0), (-1, 0), (0, 1), (0, -1), (1, 1), (1, -1), (-1, 1), (-1, -1))
    z = lax.shift_right_logical(py, 1) & 3
    y = lax.shift_right_logical(py, 3)
    lines = [at(dx, 0) for dx in (1, 2, 3)]
    lines += [(px, (((y + d) & 3) * 4 + z) * 2 + core) for d in (1, 2, 3)]
    lines += [(px, (y * 4 + ((z + d) & 3)) * 2 + core) for d in (1, 2, 3)]
    partners = [at(*d) for d in ring] + [lines[1]] + lines[3:]

    border_load = pltpu.make_async_copy(grid.at[0:GB], grid_v.at[0:GB], in_sem.at[0])
    first_weight = pltpu.make_async_copy(w0.at[0], w_v.at[0, 0], w_sem.at[0])
    small = [
        (grid.at[GB:G], grid_v.at[GB:G]), (mesh, mesh_v), (encs, encs_v), (mshs, mshs_v), (decs, decs_v),
        (v0, v_v.at[0]), (v1, v_v.at[1]), (v2, v_v.at[2]),
        (v3, v_v.at[3]), (v4, v_v.at[4]), (v5, v_v.at[5]),
    ]
    loads = [pltpu.make_async_copy(s, d, in_sem.at[i + 1]) for i, (s, d) in enumerate(small)]
    wloads = {0: pltpu.make_async_copy(w0.at[1:3], w_v.at[0, 1:3], w_sem.at[6])}
    for i, s in enumerate((w1, w2, w3, w4, w5)):
        wloads[i + 1] = pltpu.make_async_copy(s, w_v.at[i + 1], w_sem.at[i + 1])
    border_load.start()
    first_weight.start()
    barrier = pltpu.get_barrier_semaphore()
    for p in partners:
        pl.semaphore_signal(barrier, inc=1, device_id=p, device_id_type=MESH)
    for c in loads:
        c.start()
    wloads[0].start()

    def spread(buf, off, rows, value):
        for c in range(4):
            buf[pl.ds(off * 4 + c, rows, stride=4), :] = value[:, 128 * c : 128 * c + 128]

    def dot(a, b):
        return jnp.dot(a, b, preferred_element_type=F32)

    def bias(i):
        return v_v[i, 0:1, :]

    def gain(i):
        return 1.0 + v_v[i, 1:2, :]

    def centre(i):
        def some(j, carry):
            at_rows = pl.ds(pl.multiple_of(j * 128, 128), 128)
            w = w_v[i, 2, at_rows, :].astype(F32)
            w_v[i, 2, at_rows, :] = (w - jnp.mean(w, axis=1, keepdims=True)).astype(BF16)
            return carry

        lax.fori_loop(0, D // 128, some, 0)

    def border_copy(src, sx, sy, to, half):
        slot = sx * 3 + sy
        return pltpu.make_async_remote_copy(
            src_ref=src, dst_ref=rim1.at[slot, half * HALF : half * HALF + HALF],
            send_sem=s1_sem.at[slot, half], recv_sem=r1_sem.at[slot, half],
            device_id=to, device_id_type=MESH,
        )

    border_load.wait()
    first_weight.wait()
    spread(tab1, OWN, GB, dot(grid_v[0:GB, :], w_v[0, 0]) * 0.5)
    send1[...] = tab1[OWN * 4 : (OWN + GB) * 4, :].astype(BF16)
    pl.semaphore_wait(barrier, len(partners))
    along_x = [[], []]
    along_y = [[], []]
    for half in range(2):
        part = send1.at[half * HALF : half * HALF + HALF]
        for d in (1, -1):
            along_x[half].append(border_copy(part, 1 - d, 1, at(d, 0), half))
            along_y[half].append(border_copy(part, 1, 1 - d, at(0, d), half))
    for half in range(2):
        for c in along_x[half] + along_y[half]:
            c.start()
    for i in (1, 4, 5, 2, 3):
        wloads[i].start()
    for p in lines:
        pl.semaphore_signal(meet_a, inc=1, device_id=p, device_id_type=MESH)

    for c in loads:
        c.wait()
    spread(tab1, OWN + GB, G - GB, dot(grid_v[GB:G, :], w_v[0, 0]) * 0.5)
    dead = jnp.full((8, 128), -1e30, F32)
    for t in (tab1, tab2, tab3):
        t[0:8, :] = dead
    for t, rows in ((tab1, ROWS1), (tab2, ROWS2), (tab3, ROWS3)):
        t[rows * 4 : rows * 4 + 8, :] = dead

    odd = (lax.broadcasted_iota(jnp.int32, (M, K), 0) & 1) * 4
    odd3 = (lax.broadcasted_iota(jnp.int32, (K3, R3), 1) & 1) * 4

    def place(src, pos, rows, border, rim):
        pos[...] = jnp.zeros(pos.shape, jnp.int32)
        pos[:, 0:K] = rows_of(src[...], rows, border, rim, px, py).T * 4 - odd

    place(encs_v, pos1, G, GB, RIM1)
    idx_loads = [
        pltpu.make_async_copy(pos, idx, idx_sem.at[i])
        for i, (pos, idx) in enumerate(((pos1, idx1), (pos2, idx2), (pos3, idx3)))
    ]
    idx_loads[0].start()
    wloads[0].wait()
    base[...] = (dot(mesh_v[...], w_v[0, 1]) + bias(0)) * 0.5
    pl.semaphore_wait(meet_a, len(lines))
    for p in lines:
        pl.semaphore_signal(meet_b, inc=1, device_id=p, device_id_type=MESH)

    corners = [[], []]
    for half in range(2):
        for sx in (0, 2):
            part = rim1.at[sx * 3 + 1, half * HALF : half * HALF + HALF]
            for d in (1, -1):
                corners[half].append(border_copy(part, sx, 1 - d, at(0, d), half))

    for c in along_x[0]:
        c.wait_recv()
    for c in corners[0]:
        c.start()
    centre(0)
    wloads[1].wait()
    centre(1)
    nodebase[...] = dot(mesh_v[...], w_v[1, 0]) + bias(1)
    for c in along_x[1]:
        c.wait_recv()
    for c in corners[1]:
        c.start()
    place(mshs_v, pos2, M, MB, RIM2)
    pos3[...] = jnp.zeros(pos3.shape, jnp.int32)
    for b in range(BLOCKS3):
        row = rows_of(decs_v[:, R3 * b : R3 * b + R3], M, MB, RIM2, px, py)
        pos3[8 * b : 8 * b + K3, :] = row * 4 - odd3
    idx_loads[1].start()
    idx_loads[2].start()
    for i in (4, 5, 2, 3):
        wloads[i].wait()
        centre(i)
    base3[...] = (dot(grid_v[...], w_v[4, 1]) + bias(4)) * 0.5
    nodebase3[...] = dot(grid_v[...], w_v[5, 0]) + bias(5)
    coarse[core, chip] = jnp.zeros((4 * CM, 128), BF16)

    def unpack(tab, first_row, rim, slots, rows):
        for slot in slots:
            lo = (first_row + slot * rows) * 4
            tab[lo : lo + rows * 4, :] = rim[slot].astype(F32)

    unpack(tab1, RIM1, rim1, (1, 7), GB)
    for c in along_y[0] + along_y[1]:
        c.wait_recv()
    unpack(tab1, RIM1, rim1, (3, 5), GB)
    for c in corners[0] + corners[1]:
        c.wait_recv()
    unpack(tab1, RIM1, rim1, (0, 2, 6, 8), GB)
    for half in range(2):
        for c in along_x[half] + along_y[half] + corners[half]:
            c.wait_send()
    for c in idx_loads:
        c.wait()
    pl.semaphore_wait(meet_b, len(lines))

    def update(i, rows, x, agg, node, new):
        kept = {}

        def one():
            kept["p"] = node[rows, :] + dot(agg[rows, :], w_v[i, 1])

        def two():
            kept["h"] = silu_half(kept["p"] * 0.5).astype(BF16)

        def three():
            kept["o"] = dot(kept["h"], w_v[i, 2])

        def four():
            o = kept["o"]
            s = lax.rsqrt(jnp.mean(o * o, axis=1, keepdims=True) + 1e-5)
            new[rows, :] = (x[rows, :].astype(F32) + o * s * gain(i)).astype(BF16)

        return [one, two, three, four]

    low = lax.broadcasted_iota(jnp.int32, (8, 128), 0) < 4

    def gather(tab, idx, gat, slots, receivers, where):
        def some(first, k):
            for r in range(0, 16, 2):
                ia, ib = idx[where(first + r, k)], idx[where(first + r + 1, k)]
                e = first * slots + k * 16 + r
                gat[4 * e : 4 * e + 8, :] = jnp.where(low, tab[pl.ds(ia, 8), :], tab[pl.ds(ib, 8), :])

        return [functools.partial(some, first, k) for first in range(0, receivers, 16) for k in range(slots)]

    def messages(i, gat, hid, mlp, slots, receivers, base_ref, base_row, agg, side):
        edges = slots * receivers
        places = [(first, k) for first in range(0, receivers, 16) for k in range(slots)]
        half = len(places) // 2

        def hidden(first, k):
            e = first * slots + k * 16
            for c in range(4):
                cols = slice(128 * c, 128 * c + 128)
                y = gat[pl.ds(4 * e + c, 16, stride=4), :] + base_ref[base_row + first : base_row + first + 16, cols]
                hid[e : e + 16, cols] = silu_half(y).astype(BF16)

        def product(lo, hi):
            mlp[lo:hi, :] = dot(hid[lo:hi, :], w_v[i, 2])

        kept = {}

        def collect(first, k):
            e = first * slots + k * 16
            o = mlp[e : e + 16, :]
            o = o * lax.rsqrt(jnp.mean(o * o, axis=1, keepdims=True) + 1e-5)
            kept["sum"] = o if k == 0 else kept["sum"] + o
            if k == slots - 1:
                agg[base_row + first : base_row + first + 16, :] = (kept["sum"] * gain(i)).astype(BF16)

        steps = [functools.partial(hidden, *p) for p in places[:half]]
        steps.append(functools.partial(product, 0, edges // 2))
        steps += [functools.partial(hidden, *p) for p in places[half:]]
        steps.append(functools.partial(product, edges // 2, edges))
        steps += [functools.partial(collect, *p) for p in places]
        done = 0
        for n, step in enumerate(steps):
            step()
            upto = (n + 1) * len(side) // len(steps)
            for s in side[done:upto]:
                s()
            done = upto

    def mix(a, b):
        tagged = [((n + 0.5) / len(a), 0, n, s) for n, s in enumerate(a)]
        tagged += [((n + 0.5) / len(b), 1, n, s) for n, s in enumerate(b)]
        return [t[3] for t in sorted(tagged, key=lambda t: t[:3])]

    def mesh_step(i, tab, idx, extra):
        gats, hids, mlps = (gat_a, gat_b), (hid_a, hid_b), (mlp_a, mlp_b)

        def fetch(b):
            if b == BLOCKS:
                return []
            return gather(tab, idx, gats[b % 2], K, R, lambda r, k: (b * R + r, k))

        for s in fetch(0):
            s()
        for b in range(BLOCKS):
            p = b % 2
            side = fetch(b + 1)
            if b in extra:
                side = mix(side, extra[b])
            messages(i, gats[p], hids[p], mlps[p], K, R, base, b * R, aggb, side)

    def halo_copies(src, rim, s_sem, r_sem):
        return [
            pltpu.make_async_remote_copy(
                src_ref=src, dst_ref=rim.at[(1 - dx) * 3 + 1 - dy],
                send_sem=s_sem.at[(1 - dx) * 3 + 1 - dy], recv_sem=r_sem.at[(1 - dx) * 3 + 1 - dy],
                device_id=at(dx, dy), device_id_type=MESH,
            )
            for dx, dy in ring
        ]

    def coarse_copy(j):
        to = (chip + j) & (CHIPS - 1)
        return pltpu.make_async_remote_copy(
            src_ref=send2.at[0 : 4 * CM], dst_ref=coarse.at[core, chip], send_sem=sc_sem, recv_sem=rc_sem,
            device_id=(lax.shift_right_logical(to, log2(NY // 2)), (to & (NY // 2 - 1)) * 2 + core),
            device_id_type=MESH,
        )

    def coarse_all():
        return pltpu.make_async_remote_copy(
            src_ref=coarse.at[core, 0 : CHIPS - 1], dst_ref=coarse.at[core, 0 : CHIPS - 1],
            send_sem=sc_sem, recv_sem=rc_sem, device_id=at(0, 1), device_id_type=MESH,
        )

    def send_rows(lo, hi, tab, new, w, send, starts):
        def project():
            spread(tab, OWN + lo, hi - lo, dot(new[lo:hi, :], w) * 0.5)

        def pack():
            send[lo * 4 : hi * 4, :] = tab[(OWN + lo) * 4 : (OWN + hi) * 4, :].astype(BF16)

        def start():
            for c in starts():
                c.start()

        return [project, pack, start]

    mesh_step(0, tab1, idx1, {
        1: update(1, pl.ds(0, R), mesh_v, aggb, nodebase, enc_v)
        + send_rows(0, R, tab2, enc_v, w_v[2, 0], send2, lambda: [coarse_copy(j) for j in range(1, CHIPS)]),
        2: update(1, pl.ds(R, R), mesh_v, aggb, nodebase, enc_v)
        + send_rows(R, MB, tab2, enc_v, w_v[2, 0], send2, lambda: halo_copies(send2, rim2, s2_sem, r2_sem)),
    })
    for s in update(1, pl.ds(MB, M - MB), mesh_v, aggb, nodebase, enc_v):
        s()

    coarse_all().wait_recv()
    forward = pltpu.make_async_remote_copy(
        src_ref=coarse.at[core], dst_ref=coarse.at[core], send_sem=sf_sem, recv_sem=rf_sem,
        device_id=(px, py ^ 1), device_id_type=MESH,
    )
    forward.start()
    spread(tab2, OWN + MB, M - MB, dot(enc_v[MB:M, :], w_v[2, 0]) * 0.5)
    base[...] = (dot(enc_v[...], w_v[2, 1]) + bias(2)) * 0.5
    nodebase[...] = dot(enc_v[...], w_v[3, 0]) + bias(3)
    copies = halo_copies(send2, rim2, s2_sem, r2_sem)
    for c in copies:
        c.wait_recv()
    unpack(tab2, RIM2, rim2, (0, 1, 2, 3, 5, 6, 7, 8), MB)
    forward.wait_recv()
    for a in range(2):
        lo = (COARSE + a * CHIPS * CM) * 4
        tab2[lo : lo + CHIPS * CM * 4, :] = coarse[a].reshape(CHIPS * CM * 4, 128).astype(F32)
    for c in copies:
        c.wait_send()
    coarse_all().wait_send()
    forward.wait_send()

    mesh_step(2, tab2, idx2, {
        2: update(3, pl.ds(0, MB), enc_v, aggb, nodebase, prc_v)
        + send_rows(0, MB, tab3, prc_v, w_v[4, 0], send3, lambda: halo_copies(send3, rim3, s3_sem, r3_sem)),
    })
    for s in update(3, pl.ds(MB, M - MB), enc_v, aggb, nodebase, prc_v):
        s()
    put_mesh = pltpu.make_async_copy(prc_v, out_mesh, out_sem.at[0])
    put_mesh.start()

    spread(tab3, OWN + MB, M - MB, dot(prc_v[MB:M, :], w_v[4, 0]) * 0.5)
    copies = halo_copies(send3, rim3, s3_sem, r3_sem)
    for c in copies:
        c.wait_recv()
    unpack(tab3, RIM2, rim3, (0, 1, 2, 3, 5, 6, 7, 8), MB)
    for c in copies:
        c.wait_send()

    def fetch3(b):
        if b == BLOCKS3:
            return []
        return gather(tab3, idx3, (gat_a, gat_b)[b % 2], K3, R3, lambda r, k: (8 * b + k, r))

    puts = []
    for s in fetch3(0):
        s()
    for b in range(BLOCKS3):
        side = fetch3(b + 1)
        if b > 0:
            done = update(5, pl.ds((b - 1) * R3, R3), grid_v, aggb3, nodebase3, dec_v)
            side = mix(side, done) if side else done
        messages(
            4, (gat_a, gat_b)[b % 2], (hid_a, hid_b)[b % 2], (mlp_a, mlp_b)[b % 2],
            K3, R3, base3, b * R3, aggb3, side,
        )
    put_grid = [
        pltpu.make_async_copy(dec_v.at[lo:hi], out_grid.at[lo:hi], out_sem.at[1 + n])
        for n, (lo, hi) in enumerate(((0, G - R3), (G - R3, G)))
    ]
    put_grid[0].start()
    for s in update(5, pl.ds(G - R3, R3), grid_v, aggb3, nodebase3, dec_v):
        s()
    put_grid[1].start()
    put_mesh.wait()
    for c in put_grid:
        c.wait()


def per_device(*args):
    any_space = pl.BlockSpec(memory_space=pl.ANY)
    dma = pltpu.SemaphoreType.DMA
    regular = pltpu.SemaphoreType.REGULAR
    vm = pltpu.VMEM
    sm = pltpu.SMEM
    i32 = jnp.int32
    return pl.pallas_call(
        kernel,
        out_shape=(jax.ShapeDtypeStruct((G, D), BF16), jax.ShapeDtypeStruct((M, D), BF16)),
        in_specs=[any_space] * len(args),
        out_specs=(any_space, any_space),
        scratch_shapes=[
            vm((G, D), BF16), vm((M, D), BF16), vm((K, M), i32), vm((K, M), i32), vm((K3, G), i32),
            vm((6, 3, D, D), BF16), vm((6, 2, D), F32),
            vm((M, 128), i32), vm((M, 128), i32), vm((BLOCKS3 * 8, 128), i32),
            sm((M, 128), i32), sm((M, 128), i32), sm((BLOCKS3 * 8, 128), i32),
            vm((ROWS1 * 4 + 8, 128), F32), vm((ROWS2 * 4 + 8, 128), F32), vm((ROWS3 * 4 + 8, 128), F32),
            vm((M, D), F32), vm((M, D), F32), vm((G, D), F32), vm((G, D), F32),
            vm((E * 4, 128), F32), vm((E * 4, 128), F32),
            vm((E, D), BF16), vm((E, D), BF16), vm((E, D), F32), vm((E, D), F32),
            vm((M, D), BF16), vm((M, D), BF16), vm((M, D), BF16), vm((G, D), BF16), vm((G, D), BF16),
            vm((GB * 4, 128), BF16), vm((9, GB * 4, 128), BF16),
            vm((MB * 4, 128), BF16), vm((9, MB * 4, 128), BF16),
            vm((2, CHIPS, CM * 4, 128), BF16),
            vm((MB * 4, 128), BF16), vm((9, MB * 4, 128), BF16),
            dma((12,)), dma((7,)), dma((3,)), dma((3,)),
            dma((9, 2)), dma((9, 2)), dma((9,)), dma((9,)), dma((9,)), dma((9,)),
            dma, dma, dma, dma,
            regular, regular,
        ],
        compiler_params=pltpu.CompilerParams(
            collective_id=0, has_side_effects=True, vmem_limit_bytes=60 * 1024 * 1024
        ),
    )(*args)


def solution(mesh):
    assert dict(mesh.shape) == {"gx": NX, "gy": NY}
    split = P(("gx", "gy"), None)
    lists = P(None, ("gx", "gy"))
    return jax.shard_map(
        per_device,
        mesh=mesh,
        in_specs=(split, split, lists, lists, lists) + (P(),) * 12,
        out_specs=(split, split),
        check_vma=False,
    )
```

```python
import functools

import jax
import jax.numpy as jnp
from jax import lax
from jax.experimental import pallas as pl
from jax.experimental.pallas import tpu as pltpu
from jax.sharding import PartitionSpec as P

MESH = pl.DeviceIdType.MESH
F32 = jnp.float32
BF16 = jnp.bfloat16

D = 512
G = 512
M = 128
K = 32
K3 = 3
CM = 4
GB = G // 4
MB = M // 4
NX = 4
NY = 32
CHIPS = NX * NY // 2

DEAD = 1
OWN = 2
RIM1 = OWN + G
ROWS1 = RIM1 + 9 * GB
RIM2 = OWN + M
COARSE = RIM2 + 9 * MB
ROWS2 = COARSE + 2 * CHIPS * CM
ROWS3 = COARSE

R = 16
BLOCKS = M // R
E = R * K
R3 = 128
BLOCKS3 = G // R3
E3 = R3 * K3
HALF = GB * 2


def log2(n):
    bits = n.bit_length() - 1
    assert n == 1 << bits
    return bits


def rows_of(ids, rows, border, rim, px, py):
    owner = lax.shift_right_arithmetic(ids, log2(rows))
    off = ids & (rows - 1)
    ox = lax.shift_right_arithmetic(owner, log2(NY))
    oy = owner & (NY - 1)
    dx = (ox - px) & (NX - 1)
    dy = (oy - py) & (NY - 1)
    sx = jnp.where(dx == 1, 2, jnp.where(dx == NX - 1, 0, 1))
    sy = jnp.where(dy == 0, 1, jnp.where(oy == (py ^ 1), 2, 0))
    near = ((dx <= 1) | (dx == NX - 1)) & ((dy <= 1) | (dy == NY - 1)) & (off < border)
    itself = (dx == 0) & (dy == 0)
    place = (owner & 1) * CHIPS + lax.shift_right_arithmetic(owner, 1)
    far = COARSE + place * CM + (off & (CM - 1))
    row = jnp.where(near, rim + (sx * 3 + sy) * border + off, far)
    row = jnp.where(itself, OWN + off, row)
    return jnp.where(ids < 0, DEAD, row)


def silu_half(y):
    return y * jnp.tanh(y) + y


def kernel(
    grid, mesh, encs, mshs, decs, w0, v0, w1, v1, w2, v2, w3, v3, w4, v4, w5, v5,
    out_grid, out_mesh,
    grid_v, mesh_v, encs_v, mshs_v, decs_v, w_v, v_v,
    pos1, pos2, pos3, idx1, idx2, idx3,
    tab1, tab2, tab3, base, nodebase, base3, nodebase3,
    gat_a, gat_b, hid_a, hid_b, mlp_a, mlp_b,
    aggb, enc_v, prc_v, dec_v, aggb3,
    send1, rim1, send2, rim2, coarse, send3, rim3,
    in_sem, w_sem, idx_sem, out_sem,
    s1_sem, r1_sem, s2_sem, r2_sem, s3_sem, r3_sem, sc_sem, rc_sem, sf_sem, rf_sem,
    meet_a, meet_b,
):
    px = lax.axis_index("gx")
    py = lax.axis_index("gy")
    core = py & 1
    chip = px * (NY // 2) + lax.shift_right_logical(py, 1)

    def at(dx, dy):
        return ((px + dx) & (NX - 1), (py + dy) & (NY - 1))

    ring = ((1, 0), (-1, 0), (0, 1), (0, -1), (1, 1), (1, -1), (-1, 1), (-1, -1))
    z = lax.shift_right_logical(py, 1) & 3
    y = lax.shift_right_logical(py, 3)
    lines = [at(dx, 0) for dx in (1, 2, 3)]
    lines += [(px, (((y + d) & 3) * 4 + z) * 2 + core) for d in (1, 2, 3)]
    lines += [(px, (y * 4 + ((z + d) & 3)) * 2 + core) for d in (1, 2, 3)]
    partners = [at(*d) for d in ring] + [lines[1]] + lines[3:]

    border_load = pltpu.make_async_copy(grid.at[0:GB], grid_v.at[0:GB], in_sem.at[0])
    first_weight = pltpu.make_async_copy(w0.at[0], w_v.at[0, 0], w_sem.at[0])
    small = [
        (grid.at[GB:G], grid_v.at[GB:G]), (mesh, mesh_v), (encs, encs_v), (mshs, mshs_v), (decs, decs_v),
        (v0, v_v.at[0]), (v1, v_v.at[1]), (v2, v_v.at[2]),
        (v3, v_v.at[3]), (v4, v_v.at[4]), (v5, v_v.at[5]),
    ]
    loads = [pltpu.make_async_copy(s, d, in_sem.at[i + 1]) for i, (s, d) in enumerate(small)]
    wloads = {0: pltpu.make_async_copy(w0.at[1:3], w_v.at[0, 1:3], w_sem.at[6])}
    for i, s in enumerate((w1, w2, w3, w4, w5)):
        wloads[i + 1] = pltpu.make_async_copy(s, w_v.at[i + 1], w_sem.at[i + 1])
    barrier = pltpu.get_barrier_semaphore()
    for p in partners:
        pl.semaphore_signal(barrier, inc=1, device_id=p, device_id_type=MESH)
    border_load.start()
    first_weight.start()
    for c in loads:
        c.start()
    wloads[0].start()

    def spread(buf, off, rows, value):
        for c in range(4):
            buf[pl.ds(off * 4 + c, rows, stride=4), :] = value[:, 128 * c : 128 * c + 128]

    def dot(a, b):
        return jnp.dot(a, b, preferred_element_type=F32)

    def bias(i):
        return v_v[i, 0:1, :]

    def gain(i):
        return 1.0 + v_v[i, 1:2, :]

    def centre(i):
        def some(j, carry):
            at_rows = pl.ds(pl.multiple_of(j * 128, 128), 128)
            w = w_v[i, 2, at_rows, :].astype(F32)
            w_v[i, 2, at_rows, :] = (w - jnp.mean(w, axis=1, keepdims=True)).astype(BF16)
            return carry

        lax.fori_loop(0, D // 128, some, 0)

    across = 1 - 2 * (1 - core)
    sides = {0: at(0, across), 2: at(0, -across)}

    def border_copy(src, sx, sy, to, half):
        slot = sx * 3 + sy
        return pltpu.make_async_remote_copy(
            src_ref=src, dst_ref=rim1.at[slot, half * HALF : half * HALF + HALF],
            send_sem=s1_sem.at[slot, half], recv_sem=r1_sem.at[slot, half],
            device_id=to, device_id_type=MESH,
        )

    def kept_half(slot, half):
        return rim1.at[slot, half * HALF : half * HALF + HALF]

    border_load.wait()
    first_weight.wait()
    spread(tab1, OWN, GB, dot(grid_v[0:GB, :], w_v[0, 0]) * 0.5)
    send1[...] = tab1[OWN * 4 : (OWN + GB) * 4, :].astype(BF16)
    pl.semaphore_wait(barrier, len(partners))
    halves = [send1.at[h * HALF : h * HALF + HALF] for h in range(2)]
    along_x = [[border_copy(halves[h], 1 - d, 1, at(d, 0), h) for d in (1, -1)] for h in range(2)]
    aside = {(sy, h): border_copy(halves[h], 1, sy, sides[sy], h) for sy in (0, 2) for h in range(2)}
    for c in along_x[0] + [aside[0, 1]] + along_x[1] + [aside[0, 0], aside[2, 0], aside[2, 1]]:
        c.start()
    for i in (1, 4, 5, 2, 3):
        wloads[i].start()
    for p in lines:
        pl.semaphore_signal(meet_a, inc=1, device_id=p, device_id_type=MESH)

    for c in loads:
        c.wait()
    spread(tab1, OWN + GB, G - GB, dot(grid_v[GB:G, :], w_v[0, 0]) * 0.5)
    dead = jnp.full((8, 128), -1e30, F32)
    for t in (tab1, tab2, tab3):
        t[0:8, :] = dead
    for t, rows in ((tab1, ROWS1), (tab2, ROWS2), (tab3, ROWS3)):
        t[rows * 4 : rows * 4 + 8, :] = dead

    odd = (lax.broadcasted_iota(jnp.int32, (M, K), 0) & 1) * 4
    odd3 = (lax.broadcasted_iota(jnp.int32, (K3, R3), 1) & 1) * 4

    def place(src, pos, rows, border, rim):
        pos[...] = jnp.zeros(pos.shape, jnp.int32)
        pos[:, 0:K] = rows_of(src[...], rows, border, rim, px, py).T * 4 - odd

    place(encs_v, pos1, G, GB, RIM1)
    idx_loads = [
        pltpu.make_async_copy(pos, idx, idx_sem.at[i])
        for i, (pos, idx) in enumerate(((pos1, idx1), (pos2, idx2), (pos3, idx3)))
    ]
    idx_loads[0].start()
    wloads[0].wait()
    base[...] = (dot(mesh_v[...], w_v[0, 1]) + bias(0)) * 0.5

    to_core = [[border_copy(kept_half(sx * 3 + 1, h), sx, 2, sides[2], h) for sx in (0, 2)] for h in range(2)]
    to_chip = [border_copy(kept_half(sx * 3 + 1, 0), sx, 0, sides[0], 0) for sx in (0, 2)]
    to_x = [border_copy(kept_half(3, 1), 1 - d, 0, at(d, 0), 1) for d in (1, -1)]

    for c in along_x[0]:
        c.wait_recv()
    for c in to_chip + to_core[0]:
        c.start()
    centre(0)
    wloads[1].wait()
    centre(1)
    nodebase[...] = dot(mesh_v[...], w_v[1, 0]) + bias(1)
    aside[0, 1].wait_recv()
    for c in to_x:
        c.start()
    for c in along_x[1]:
        c.wait_recv()
    for c in to_core[1]:
        c.start()
    pl.semaphore_wait(meet_a, len(lines))
    for p in lines:
        pl.semaphore_signal(meet_b, inc=1, device_id=p, device_id_type=MESH)
    place(mshs_v, pos2, M, MB, RIM2)
    pos3[...] = jnp.zeros(pos3.shape, jnp.int32)
    for b in range(BLOCKS3):
        row = rows_of(decs_v[:, R3 * b : R3 * b + R3], M, MB, RIM2, px, py)
        pos3[8 * b : 8 * b + K3, :] = row * 4 - odd3
    idx_loads[1].start()
    idx_loads[2].start()
    for i in (4, 5, 2, 3):
        wloads[i].wait()
        centre(i)
    base3[...] = (dot(grid_v[...], w_v[4, 1]) + bias(4)) * 0.5
    nodebase3[...] = dot(grid_v[...], w_v[5, 0]) + bias(5)
    coarse[core, chip] = jnp.zeros((4 * CM, 128), BF16)

    def unpack(tab, first_row, rim, slots, rows):
        for slot in slots:
            lo = (first_row + slot * rows) * 4
            tab[lo : lo + rows * 4, :] = rim[slot].astype(F32)

    unpack(tab1, RIM1, rim1, (1, 7), GB)
    for c in to_core[0] + to_core[1] + [aside[0, 0], aside[2, 0], aside[2, 1]]:
        c.wait_recv()
    unpack(tab1, RIM1, rim1, (3, 5, 2, 8), GB)
    for c in to_chip + to_x:
        c.wait_recv()
    unpack(tab1, RIM1, rim1, (0, 6), GB)
    for c in idx_loads:
        c.wait()

    def update(i, rows, x, agg, node, new):
        kept = {}

        def one():
            kept["p"] = node[rows, :] + dot(agg[rows, :], w_v[i, 1])

        def two():
            kept["h"] = silu_half(kept["p"] * 0.5).astype(BF16)

        def three():
            kept["o"] = dot(kept["h"], w_v[i, 2])

        def four():
            o = kept["o"]
            s = lax.rsqrt(jnp.mean(o * o, axis=1, keepdims=True) + 1e-5)
            new[rows, :] = (x[rows, :].astype(F32) + o * s * gain(i)).astype(BF16)

        return [one, two, three, four]

    low = lax.broadcasted_iota(jnp.int32, (8, 128), 0) < 4

    def gather(tab, idx, gat, slots, receivers, where):
        def some(first, k):
            for r in range(0, 16, 2):
                ia, ib = idx[where(first + r, k)], idx[where(first + r + 1, k)]
                e = first * slots + k * 16 + r
                gat[4 * e : 4 * e + 8, :] = jnp.where(low, tab[pl.ds(ia, 8), :], tab[pl.ds(ib, 8), :])

        return [functools.partial(some, first, k) for first in range(0, receivers, 16) for k in range(slots)]

    def messages(i, gat, hid, mlp, slots, receivers, base_ref, base_row, agg, side):
        edges = slots * receivers
        places = [(first, k) for first in range(0, receivers, 16) for k in range(slots)]
        half = len(places) // 2

        def hidden(first, k):
            e = first * slots + k * 16
            for c in range(4):
                cols = slice(128 * c, 128 * c + 128)
                y = gat[pl.ds(4 * e + c, 16, stride=4), :] + base_ref[base_row + first : base_row + first + 16, cols]
                hid[e : e + 16, cols] = silu_half(y).astype(BF16)

        def product(lo, hi):
            mlp[lo:hi, :] = dot(hid[lo:hi, :], w_v[i, 2])

        kept = {}

        def collect(first, k):
            e = first * slots + k * 16
            o = mlp[e : e + 16, :]
            o = o * lax.rsqrt(jnp.mean(o * o, axis=1, keepdims=True) + 1e-5)
            kept["sum"] = o if k == 0 else kept["sum"] + o
            if k == slots - 1:
                agg[base_row + first : base_row + first + 16, :] = (kept["sum"] * gain(i)).astype(BF16)

        steps = [functools.partial(hidden, *p) for p in places[:half]]
        steps.append(functools.partial(product, 0, edges // 2))
        steps += [functools.partial(hidden, *p) for p in places[half:]]
        steps.append(functools.partial(product, edges // 2, edges))
        steps += [functools.partial(collect, *p) for p in places]
        done = 0
        for n, step in enumerate(steps):
            step()
            upto = (n + 1) * len(side) // len(steps)
            for s in side[done:upto]:
                s()
            done = upto

    def mix(a, b):
        tagged = [((n + 0.5) / len(a), 0, n, s) for n, s in enumerate(a)]
        tagged += [((n + 0.5) / len(b), 1, n, s) for n, s in enumerate(b)]
        return [t[3] for t in sorted(tagged, key=lambda t: t[:3])]

    def mesh_step(i, tab, idx, extra):
        gats, hids, mlps = (gat_a, gat_b), (hid_a, hid_b), (mlp_a, mlp_b)

        def fetch(b):
            if b == BLOCKS:
                return []
            return gather(tab, idx, gats[b % 2], K, R, lambda r, k: (b * R + r, k))

        for s in fetch(0):
            s()
        for b in range(BLOCKS):
            p = b % 2
            side = fetch(b + 1)
            if b in extra:
                side = mix(side, extra[b])
            messages(i, gats[p], hids[p], mlps[p], K, R, base, b * R, aggb, side)

    def halo_copies(src, rim, s_sem, r_sem):
        copies = []
        for dx, sy in ((1, 0), (-1, 0), (0, 0), (1, 1), (-1, 1), (1, 2), (-1, 2), (0, 2)):
            slot = (1 - dx) * 3 + sy
            copies.append(
                pltpu.make_async_remote_copy(
                    src_ref=src, dst_ref=rim.at[slot], send_sem=s_sem.at[slot], recv_sem=r_sem.at[slot],
                    device_id=at(dx, (0 if sy == 1 else across if sy == 0 else -across)), device_id_type=MESH,
                )
            )
        return copies

    def coarse_copy(j):
        to = (chip + j) & (CHIPS - 1)
        return pltpu.make_async_remote_copy(
            src_ref=send2.at[0 : 4 * CM], dst_ref=coarse.at[core, chip], send_sem=sc_sem, recv_sem=rc_sem,
            device_id=(lax.shift_right_logical(to, log2(NY // 2)), (to & (NY // 2 - 1)) * 2 + core),
            device_id_type=MESH,
        )

    def coarse_all():
        return pltpu.make_async_remote_copy(
            src_ref=coarse.at[core, 0 : CHIPS - 1], dst_ref=coarse.at[core, 0 : CHIPS - 1],
            send_sem=sc_sem, recv_sem=rc_sem, device_id=at(0, 1), device_id_type=MESH,
        )

    def all_coarse():
        pl.semaphore_wait(meet_b, len(lines))
        return [coarse_copy(j) for j in range(1, CHIPS)]

    def send_rows(lo, hi, tab, new, w, send, starts):
        def project():
            spread(tab, OWN + lo, hi - lo, dot(new[lo:hi, :], w) * 0.5)

        def pack():
            send[lo * 4 : hi * 4, :] = tab[(OWN + lo) * 4 : (OWN + hi) * 4, :].astype(BF16)

        def start():
            for c in starts():
                c.start()

        return [project, pack, start]

    mesh_step(0, tab1, idx1, {
        1: update(1, pl.ds(0, R), mesh_v, aggb, nodebase, enc_v)
        + send_rows(0, R, tab2, enc_v, w_v[2, 0], send2, all_coarse),
        2: update(1, pl.ds(R, R), mesh_v, aggb, nodebase, enc_v)
        + send_rows(R, MB, tab2, enc_v, w_v[2, 0], send2, lambda: halo_copies(send2, rim2, s2_sem, r2_sem)),
    })
    for s in update(1, pl.ds(MB, M - MB), mesh_v, aggb, nodebase, enc_v):
        s()

    for c in along_x[0] + along_x[1] + list(aside.values()) + to_core[0] + to_core[1] + to_chip + to_x:
        c.wait_send()

    coarse_all().wait_recv()
    forward = pltpu.make_async_remote_copy(
        src_ref=coarse.at[core], dst_ref=coarse.at[core], send_sem=sf_sem, recv_sem=rf_sem,
        device_id=(px, py ^ 1), device_id_type=MESH,
    )
    forward.start()
    spread(tab2, OWN + MB, M - MB, dot(enc_v[MB:M, :], w_v[2, 0]) * 0.5)
    base[...] = (dot(enc_v[...], w_v[2, 1]) + bias(2)) * 0.5
    nodebase[...] = dot(enc_v[...], w_v[3, 0]) + bias(3)
    copies = halo_copies(send2, rim2, s2_sem, r2_sem)
    for c in copies:
        c.wait_recv()
    unpack(tab2, RIM2, rim2, (0, 1, 2, 3, 5, 6, 7, 8), MB)
    forward.wait_recv()
    for a in range(2):
        lo = (COARSE + a * CHIPS * CM) * 4
        tab2[lo : lo + CHIPS * CM * 4, :] = coarse[a].reshape(CHIPS * CM * 4, 128).astype(F32)
    for c in copies:
        c.wait_send()
    coarse_all().wait_send()
    forward.wait_send()

    mesh_step(2, tab2, idx2, {
        2: update(3, pl.ds(0, MB), enc_v, aggb, nodebase, prc_v)
        + send_rows(0, MB, tab3, prc_v, w_v[4, 0], send3, lambda: halo_copies(send3, rim3, s3_sem, r3_sem)),
    })
    for s in update(3, pl.ds(MB, M - MB), enc_v, aggb, nodebase, prc_v):
        s()
    put_mesh = pltpu.make_async_copy(prc_v, out_mesh, out_sem.at[0])
    put_mesh.start()

    spread(tab3, OWN + MB, M - MB, dot(prc_v[MB:M, :], w_v[4, 0]) * 0.5)
    copies = halo_copies(send3, rim3, s3_sem, r3_sem)
    for c in copies:
        c.wait_recv()
    unpack(tab3, RIM2, rim3, (0, 1, 2, 3, 5, 6, 7, 8), MB)
    for c in copies:
        c.wait_send()

    def fetch3(b):
        if b == BLOCKS3:
            return []
        return gather(tab3, idx3, (gat_a, gat_b)[b % 2], K3, R3, lambda r, k: (8 * b + k, r))

    puts = []
    for s in fetch3(0):
        s()
    for b in range(BLOCKS3):
        side = fetch3(b + 1)
        if b > 0:
            done = update(5, pl.ds((b - 1) * R3, R3), grid_v, aggb3, nodebase3, dec_v)
            side = mix(side, done) if side else done
        messages(
            4, (gat_a, gat_b)[b % 2], (hid_a, hid_b)[b % 2], (mlp_a, mlp_b)[b % 2],
            K3, R3, base3, b * R3, aggb3, side,
        )
    put_grid = [
        pltpu.make_async_copy(dec_v.at[lo:hi], out_grid.at[lo:hi], out_sem.at[1 + n])
        for n, (lo, hi) in enumerate(((0, G - R3), (G - R3, G)))
    ]
    put_grid[0].start()
    for s in update(5, pl.ds(G - R3, R3), grid_v, aggb3, nodebase3, dec_v):
        s()
    put_grid[1].start()
    put_mesh.wait()
    for c in put_grid:
        c.wait()


def per_device(*args):
    any_space = pl.BlockSpec(memory_space=pl.ANY)
    dma = pltpu.SemaphoreType.DMA
    regular = pltpu.SemaphoreType.REGULAR
    vm = pltpu.VMEM
    sm = pltpu.SMEM
    i32 = jnp.int32
    return pl.pallas_call(
        kernel,
        out_shape=(jax.ShapeDtypeStruct((G, D), BF16), jax.ShapeDtypeStruct((M, D), BF16)),
        in_specs=[any_space] * len(args),
        out_specs=(any_space, any_space),
        scratch_shapes=[
            vm((G, D), BF16), vm((M, D), BF16), vm((K, M), i32), vm((K, M), i32), vm((K3, G), i32),
            vm((6, 3, D, D), BF16), vm((6, 2, D), F32),
            vm((M, 128), i32), vm((M, 128), i32), vm((BLOCKS3 * 8, 128), i32),
            sm((M, 128), i32), sm((M, 128), i32), sm((BLOCKS3 * 8, 128), i32),
            vm((ROWS1 * 4 + 8, 128), F32), vm((ROWS2 * 4 + 8, 128), F32), vm((ROWS3 * 4 + 8, 128), F32),
            vm((M, D), F32), vm((M, D), F32), vm((G, D), F32), vm((G, D), F32),
            vm((E * 4, 128), F32), vm((E * 4, 128), F32),
            vm((E, D), BF16), vm((E, D), BF16), vm((E, D), F32), vm((E, D), F32),
            vm((M, D), BF16), vm((M, D), BF16), vm((M, D), BF16), vm((G, D), BF16), vm((G, D), BF16),
            vm((GB * 4, 128), BF16), vm((9, GB * 4, 128), BF16),
            vm((MB * 4, 128), BF16), vm((9, MB * 4, 128), BF16),
            vm((2, CHIPS, CM * 4, 128), BF16),
            vm((MB * 4, 128), BF16), vm((9, MB * 4, 128), BF16),
            dma((12,)), dma((7,)), dma((3,)), dma((3,)),
            dma((9, 2)), dma((9, 2)), dma((9,)), dma((9,)), dma((9,)), dma((9,)),
            dma, dma, dma, dma,
            regular, regular,
        ],
        compiler_params=pltpu.CompilerParams(
            collective_id=0, has_side_effects=True, vmem_limit_bytes=60 * 1024 * 1024
        ),
    )(*args)


def solution(mesh):
    assert dict(mesh.shape) == {"gx": NX, "gy": NY}
    split = P(("gx", "gy"), None)
    lists = P(None, ("gx", "gy"))
    return jax.shard_map(
        per_device,
        mesh=mesh,
        in_specs=(split, split, lists, lists, lists) + (P(),) * 12,
        out_specs=(split, split),
        check_vma=False,
    )
```

```python
import functools

import jax
import jax.numpy as jnp
from jax import lax
from jax.experimental import pallas as pl
from jax.experimental.pallas import tpu as pltpu
from jax.sharding import PartitionSpec as P

MESH = pl.DeviceIdType.MESH
F32 = jnp.float32
BF16 = jnp.bfloat16

D = 512
G = 512
M = 128
K = 32
K3 = 3
CM = 4
GB = G // 4
MB = M // 4
NX = 4
NY = 32
CHIPS = NX * NY // 2

DEAD = 1
OWN = 2
RIM1 = OWN + G
ROWS1 = RIM1 + 9 * GB
RIM2 = OWN + M
COARSE = RIM2 + 9 * MB
ROWS2 = COARSE + 2 * CHIPS * CM
ROWS3 = COARSE

R = 16
BLOCKS = M // R
E = R * K
R3 = 128
BLOCKS3 = G // R3
E3 = R3 * K3
HALF = GB * 2


def log2(n):
    bits = n.bit_length() - 1
    assert n == 1 << bits
    return bits


def rows_of(ids, rows, border, rim, px, py):
    owner = lax.shift_right_arithmetic(ids, log2(rows))
    off = ids & (rows - 1)
    ox = lax.shift_right_arithmetic(owner, log2(NY))
    oy = owner & (NY - 1)
    dx = (ox - px) & (NX - 1)
    dy = (oy - py) & (NY - 1)
    sx = jnp.where(dx == 1, 2, jnp.where(dx == NX - 1, 0, 1))
    sy = jnp.where(dy == 0, 1, jnp.where(oy == (py ^ 1), 2, 0))
    near = ((dx <= 1) | (dx == NX - 1)) & ((dy <= 1) | (dy == NY - 1)) & (off < border)
    itself = (dx == 0) & (dy == 0)
    place = (owner & 1) * CHIPS + lax.shift_right_arithmetic(owner, 1)
    far = COARSE + place * CM + (off & (CM - 1))
    row = jnp.where(near, rim + (sx * 3 + sy) * border + off, far)
    row = jnp.where(itself, OWN + off, row)
    return jnp.where(ids < 0, DEAD, row)


def silu_half(y):
    return y * jnp.tanh(y) + y


def kernel(
    grid, mesh, encs, mshs, decs, w0, v0, w1, v1, w2, v2, w3, v3, w4, v4, w5, v5,
    out_grid, out_mesh,
    grid_v, mesh_v, encs_v, mshs_v, decs_v, w_v, v_v,
    pos1, pos2, pos3, idx1, idx2, idx3,
    tab1, tab2, tab3, base, nodebase, base3, nodebase3,
    gat_a, gat_b, hid_a, hid_b, mlp_a, mlp_b,
    aggb, enc_v, prc_v, dec_v, aggb3,
    send1, rim1, send2, rim2, coarse, send3, rim3,
    in_sem, w_sem, idx_sem, out_sem,
    s1_sem, r1_sem, s2_sem, r2_sem, s3_sem, r3_sem, sc_sem, rc_sem, sf_sem, rf_sem,
    meet_a, meet_b,
):
    px = lax.axis_index("gx")
    py = lax.axis_index("gy")
    core = py & 1
    chip = px * (NY // 2) + lax.shift_right_logical(py, 1)

    def at(dx, dy):
        return ((px + dx) & (NX - 1), (py + dy) & (NY - 1))

    ring = ((1, 0), (-1, 0), (0, 1), (0, -1), (1, 1), (1, -1), (-1, 1), (-1, -1))
    z = lax.shift_right_logical(py, 1) & 3
    y = lax.shift_right_logical(py, 3)
    lines = [at(dx, 0) for dx in (1, 2, 3)]
    lines += [(px, (((y + d) & 3) * 4 + z) * 2 + core) for d in (1, 2, 3)]
    lines += [(px, (y * 4 + ((z + d) & 3)) * 2 + core) for d in (1, 2, 3)]
    partners = [at(*d) for d in ring] + [lines[1]] + lines[3:]

    border_load = pltpu.make_async_copy(grid.at[0:GB], grid_v.at[0:GB], in_sem.at[0])
    first_weight = pltpu.make_async_copy(w0.at[0], w_v.at[0, 0], w_sem.at[0])
    small = [
        (grid.at[GB:G], grid_v.at[GB:G]), (mesh, mesh_v), (encs, encs_v), (mshs, mshs_v), (decs, decs_v),
        (v0, v_v.at[0]), (v1, v_v.at[1]), (v2, v_v.at[2]),
        (v3, v_v.at[3]), (v4, v_v.at[4]), (v5, v_v.at[5]),
    ]
    loads = [pltpu.make_async_copy(s, d, in_sem.at[i + 1]) for i, (s, d) in enumerate(small)]
    wloads = {0: pltpu.make_async_copy(w0.at[1:3], w_v.at[0, 1:3], w_sem.at[6])}
    for i, s in enumerate((w1, w2, w3, w4, w5)):
        wloads[i + 1] = pltpu.make_async_copy(s, w_v.at[i + 1], w_sem.at[i + 1])
    barrier = pltpu.get_barrier_semaphore()
    for p in partners:
        pl.semaphore_signal(barrier, inc=1, device_id=p, device_id_type=MESH)
    border_load.start()
    first_weight.start()
    for c in loads:
        c.start()
    wloads[0].start()

    def spread(buf, off, rows, value):
        for c in range(4):
            buf[pl.ds(off * 4 + c, rows, stride=4), :] = value[:, 128 * c : 128 * c + 128]

    def dot(a, b):
        return jnp.dot(a, b, preferred_element_type=F32)

    def bias(i):
        return v_v[i, 0:1, :]

    def gain(i):
        return 1.0 + v_v[i, 1:2, :]

    def centre(i):
        def some(j, carry):
            at_rows = pl.ds(pl.multiple_of(j * 128, 128), 128)
            w = w_v[i, 2, at_rows, :].astype(F32)
            w_v[i, 2, at_rows, :] = (w - jnp.mean(w, axis=1, keepdims=True)).astype(BF16)
            return carry

        lax.fori_loop(0, D // 128, some, 0)

    across = 1 - 2 * (1 - core)
    sides = {0: at(0, across), 2: at(0, -across)}

    def border_copy(src, sx, sy, to, half):
        slot = sx * 3 + sy
        return pltpu.make_async_remote_copy(
            src_ref=src, dst_ref=rim1.at[slot, half * HALF : half * HALF + HALF],
            send_sem=s1_sem.at[slot, half], recv_sem=r1_sem.at[slot, half],
            device_id=to, device_id_type=MESH,
        )

    def kept_half(slot, half):
        return rim1.at[slot, half * HALF : half * HALF + HALF]

    border_load.wait()
    first_weight.wait()
    spread(tab1, OWN, GB, dot(grid_v[0:GB, :], w_v[0, 0]) * 0.5)
    send1[...] = tab1[OWN * 4 : (OWN + GB) * 4, :].astype(BF16)
    pl.semaphore_wait(barrier, len(partners))
    halves = [send1.at[h * HALF : h * HALF + HALF] for h in range(2)]
    along_x = [[border_copy(halves[h], 1 - d, 1, at(d, 0), h) for d in (1, -1)] for h in range(2)]
    aside = {(sy, h): border_copy(halves[h], 1, sy, sides[sy], h) for sy in (0, 2) for h in range(2)}
    for c in along_x[0] + [aside[0, 1]] + along_x[1] + [aside[0, 0], aside[2, 0], aside[2, 1]]:
        c.start()
    for i in (1, 4, 5, 2, 3):
        wloads[i].start()
    for p in lines:
        pl.semaphore_signal(meet_a, inc=1, device_id=p, device_id_type=MESH)

    for c in loads:
        c.wait()
    spread(tab1, OWN + GB, G - GB, dot(grid_v[GB:G, :], w_v[0, 0]) * 0.5)
    dead = jnp.full((8, 128), -1e30, F32)
    for t in (tab1, tab2, tab3):
        t[0:8, :] = dead
    for t, rows in ((tab1, ROWS1), (tab2, ROWS2), (tab3, ROWS3)):
        t[rows * 4 : rows * 4 + 8, :] = dead

    odd = (lax.broadcasted_iota(jnp.int32, (M, K), 0) & 1) * 4
    odd3 = (lax.broadcasted_iota(jnp.int32, (K3, R3), 1) & 1) * 4

    def place(src, pos, rows, border, rim):
        pos[...] = jnp.zeros(pos.shape, jnp.int32)
        pos[:, 0:K] = rows_of(src[...], rows, border, rim, px, py).T * 4 - odd

    place(encs_v, pos1, G, GB, RIM1)
    idx_loads = [
        pltpu.make_async_copy(pos, idx, idx_sem.at[i])
        for i, (pos, idx) in enumerate(((pos1, idx1), (pos2, idx2), (pos3, idx3)))
    ]
    idx_loads[0].start()
    wloads[0].wait()
    base[...] = (dot(mesh_v[...], w_v[0, 1]) + bias(0)) * 0.5

    to_core = [[border_copy(kept_half(sx * 3 + 1, h), sx, 2, sides[2], h) for sx in (0, 2)] for h in range(2)]
    to_chip = [border_copy(kept_half(sx * 3 + 1, 0), sx, 0, sides[0], 0) for sx in (0, 2)]
    to_x = [border_copy(kept_half(3, 1), 1 - d, 0, at(d, 0), 1) for d in (1, -1)]

    for c in along_x[0]:
        c.wait_recv()
    for c in to_chip + to_core[0]:
        c.start()
    centre(0)
    wloads[1].wait()
    centre(1)
    nodebase[...] = dot(mesh_v[...], w_v[1, 0]) + bias(1)
    aside[0, 1].wait_recv()
    for c in to_x:
        c.start()
    for c in along_x[1]:
        c.wait_recv()
    for c in to_core[1]:
        c.start()
    pl.semaphore_wait(meet_a, len(lines))
    for p in lines:
        pl.semaphore_signal(meet_b, inc=1, device_id=p, device_id_type=MESH)
    place(mshs_v, pos2, M, MB, RIM2)
    pos3[...] = jnp.zeros(pos3.shape, jnp.int32)
    for b in range(BLOCKS3):
        row = rows_of(decs_v[:, R3 * b : R3 * b + R3], M, MB, RIM2, px, py)
        pos3[8 * b : 8 * b + K3, :] = row * 4 - odd3
    idx_loads[1].start()
    idx_loads[2].start()
    for i in (4, 5, 2, 3):
        wloads[i].wait()
        centre(i)
    base3[...] = (dot(grid_v[...], w_v[4, 1]) + bias(4)) * 0.5
    nodebase3[...] = dot(grid_v[...], w_v[5, 0]) + bias(5)
    coarse[core, chip] = jnp.zeros((4 * CM, 128), BF16)

    def unpack(tab, first_row, rim, slots, rows):
        for slot in slots:
            lo = (first_row + slot * rows) * 4
            tab[lo : lo + rows * 4, :] = rim[slot].astype(F32)

    unpack(tab1, RIM1, rim1, (1, 7), GB)
    for c in to_core[0] + to_core[1] + [aside[0, 0], aside[2, 0], aside[2, 1]]:
        c.wait_recv()
    unpack(tab1, RIM1, rim1, (3, 5, 2, 8), GB)
    for c in to_chip + to_x:
        c.wait_recv()
    unpack(tab1, RIM1, rim1, (0, 6), GB)
    for c in idx_loads:
        c.wait()

    def update(i, rows, x, agg, node, new):
        kept = {}

        def one():
            kept["p"] = node[rows, :] + dot(agg[rows, :], w_v[i, 1])

        def two():
            kept["h"] = silu_half(kept["p"] * 0.5).astype(BF16)

        def three():
            kept["o"] = dot(kept["h"], w_v[i, 2])

        def four():
            o = kept["o"]
            s = lax.rsqrt(jnp.mean(o * o, axis=1, keepdims=True) + 1e-5)
            new[rows, :] = (x[rows, :].astype(F32) + o * s * gain(i)).astype(BF16)

        return [one, two, three, four]

    low = lax.broadcasted_iota(jnp.int32, (8, 128), 0) < 4

    def gather(tab, idx, gat, slots, receivers, where):
        def some(first, k):
            for r in range(0, 16, 2):
                ia, ib = idx[where(first + r, k)], idx[where(first + r + 1, k)]
                e = first * slots + k * 16 + r
                gat[4 * e : 4 * e + 8, :] = jnp.where(low, tab[pl.ds(ia, 8), :], tab[pl.ds(ib, 8), :])

        return [functools.partial(some, first, k) for first in range(0, receivers, 16) for k in range(slots)]

    def messages(i, gat, hid, mlp, slots, receivers, base_ref, base_row, agg, side):
        edges = slots * receivers
        places = [(first, k) for first in range(0, receivers, 16) for k in range(slots)]
        half = len(places) // 2

        bases = {}

        def hidden(first, k):
            e = first * slots + k * 16
            if k == 0:
                bases[first] = base_ref[base_row + first : base_row + first + 16, :]
            for c in range(4):
                cols = slice(128 * c, 128 * c + 128)
                y = gat[pl.ds(4 * e + c, 16, stride=4), :] + bases[first][:, cols]
                hid[e : e + 16, cols] = silu_half(y).astype(BF16)

        def product(lo, hi):
            mlp[lo:hi, :] = dot(hid[lo:hi, :], w_v[i, 2])

        kept = {}

        def collect(first, k):
            e = first * slots + k * 16
            o = mlp[e : e + 16, :]
            o = o * lax.rsqrt(jnp.mean(o * o, axis=1, keepdims=True) + 1e-5)
            kept["sum"] = o if k == 0 else kept["sum"] + o
            if k == slots - 1:
                agg[base_row + first : base_row + first + 16, :] = (kept["sum"] * gain(i)).astype(BF16)

        steps = [functools.partial(hidden, *p) for p in places[:half]]
        steps.append(functools.partial(product, 0, edges // 2))
        steps += [functools.partial(hidden, *p) for p in places[half:]]
        steps.append(functools.partial(product, edges // 2, edges))
        steps += [functools.partial(collect, *p) for p in places]
        done = 0
        for n, step in enumerate(steps):
            step()
            upto = (n + 1) * len(side) // len(steps)
            for s in side[done:upto]:
                s()
            done = upto

    def mix(a, b):
        tagged = [((n + 0.5) / len(a), 0, n, s) for n, s in enumerate(a)]
        tagged += [((n + 0.5) / len(b), 1, n, s) for n, s in enumerate(b)]
        return [t[3] for t in sorted(tagged, key=lambda t: t[:3])]

    def mesh_step(i, tab, idx, extra):
        gats, hids, mlps = (gat_a, gat_b), (hid_a, hid_b), (mlp_a, mlp_b)

        def fetch(b):
            if b == BLOCKS:
                return []
            return gather(tab, idx, gats[b % 2], K, R, lambda r, k: (b * R + r, k))

        for s in fetch(0):
            s()
        for b in range(BLOCKS):
            p = b % 2
            side = fetch(b + 1)
            if b in extra:
                side = mix(side, extra[b])
            messages(i, gats[p], hids[p], mlps[p], K, R, base, b * R, aggb, side)

    def halo_copies(src, rim, s_sem, r_sem):
        copies = []
        for dx, sy in ((1, 0), (-1, 0), (0, 0), (1, 1), (-1, 1), (1, 2), (-1, 2), (0, 2)):
            slot = (1 - dx) * 3 + sy
            copies.append(
                pltpu.make_async_remote_copy(
                    src_ref=src, dst_ref=rim.at[slot], send_sem=s_sem.at[slot], recv_sem=r_sem.at[slot],
                    device_id=at(dx, (0 if sy == 1 else across if sy == 0 else -across)), device_id_type=MESH,
                )
            )
        return copies

    def coarse_copy(j):
        to = (chip + j) & (CHIPS - 1)
        return pltpu.make_async_remote_copy(
            src_ref=send2.at[0 : 4 * CM], dst_ref=coarse.at[core, chip], send_sem=sc_sem, recv_sem=rc_sem,
            device_id=(lax.shift_right_logical(to, log2(NY // 2)), (to & (NY // 2 - 1)) * 2 + core),
            device_id_type=MESH,
        )

    def coarse_all():
        return pltpu.make_async_remote_copy(
            src_ref=coarse.at[core, 0 : CHIPS - 1], dst_ref=coarse.at[core, 0 : CHIPS - 1],
            send_sem=sc_sem, recv_sem=rc_sem, device_id=at(0, 1), device_id_type=MESH,
        )

    def all_coarse():
        pl.semaphore_wait(meet_b, len(lines))
        return [coarse_copy(j) for j in range(1, CHIPS)]

    def send_rows(lo, hi, tab, new, w, send, starts):
        def project():
            spread(tab, OWN + lo, hi - lo, dot(new[lo:hi, :], w) * 0.5)

        def pack():
            send[lo * 4 : hi * 4, :] = tab[(OWN + lo) * 4 : (OWN + hi) * 4, :].astype(BF16)

        def start():
            for c in starts():
                c.start()

        return [project, pack, start]

    mesh_step(0, tab1, idx1, {
        1: update(1, pl.ds(0, R), mesh_v, aggb, nodebase, enc_v)
        + send_rows(0, R, tab2, enc_v, w_v[2, 0], send2, all_coarse),
        2: update(1, pl.ds(R, R), mesh_v, aggb, nodebase, enc_v)
        + send_rows(R, MB, tab2, enc_v, w_v[2, 0], send2, lambda: halo_copies(send2, rim2, s2_sem, r2_sem)),
    })
    for s in update(1, pl.ds(MB, M - MB), mesh_v, aggb, nodebase, enc_v):
        s()

    for c in along_x[0] + along_x[1] + list(aside.values()) + to_core[0] + to_core[1] + to_chip + to_x:
        c.wait_send()

    coarse_all().wait_recv()
    forward = pltpu.make_async_remote_copy(
        src_ref=coarse.at[core], dst_ref=coarse.at[core], send_sem=sf_sem, recv_sem=rf_sem,
        device_id=(px, py ^ 1), device_id_type=MESH,
    )
    forward.start()
    spread(tab2, OWN + MB, M - MB, dot(enc_v[MB:M, :], w_v[2, 0]) * 0.5)
    base[...] = (dot(enc_v[...], w_v[2, 1]) + bias(2)) * 0.5
    nodebase[...] = dot(enc_v[...], w_v[3, 0]) + bias(3)
    copies = halo_copies(send2, rim2, s2_sem, r2_sem)
    for c in copies:
        c.wait_recv()
    unpack(tab2, RIM2, rim2, (0, 1, 2, 3, 5, 6, 7, 8), MB)
    forward.wait_recv()
    for a in range(2):
        lo = (COARSE + a * CHIPS * CM) * 4
        tab2[lo : lo + CHIPS * CM * 4, :] = coarse[a].reshape(CHIPS * CM * 4, 128).astype(F32)
    for c in copies:
        c.wait_send()
    coarse_all().wait_send()
    forward.wait_send()

    mesh_step(2, tab2, idx2, {
        2: update(3, pl.ds(0, MB), enc_v, aggb, nodebase, prc_v)
        + send_rows(0, MB, tab3, prc_v, w_v[4, 0], send3, lambda: halo_copies(send3, rim3, s3_sem, r3_sem)),
    })
    for s in update(3, pl.ds(MB, M - MB), enc_v, aggb, nodebase, prc_v):
        s()
    put_mesh = pltpu.make_async_copy(prc_v, out_mesh, out_sem.at[0])
    put_mesh.start()

    spread(tab3, OWN + MB, M - MB, dot(prc_v[MB:M, :], w_v[4, 0]) * 0.5)
    copies = halo_copies(send3, rim3, s3_sem, r3_sem)
    for c in copies:
        c.wait_recv()
    unpack(tab3, RIM2, rim3, (0, 1, 2, 3, 5, 6, 7, 8), MB)
    for c in copies:
        c.wait_send()

    def fetch3(b):
        if b == BLOCKS3:
            return []
        return gather(tab3, idx3, (gat_a, gat_b)[b % 2], K3, R3, lambda r, k: (8 * b + k, r))

    puts = []
    for s in fetch3(0):
        s()
    for b in range(BLOCKS3):
        side = fetch3(b + 1)
        if b > 0:
            done = update(5, pl.ds((b - 1) * R3, R3), grid_v, aggb3, nodebase3, dec_v)
            side = mix(side, done) if side else done
        messages(
            4, (gat_a, gat_b)[b % 2], (hid_a, hid_b)[b % 2], (mlp_a, mlp_b)[b % 2],
            K3, R3, base3, b * R3, aggb3, side,
        )
    put_grid = [
        pltpu.make_async_copy(dec_v.at[lo:hi], out_grid.at[lo:hi], out_sem.at[1 + n])
        for n, (lo, hi) in enumerate(((0, G - R3), (G - R3, G)))
    ]
    put_grid[0].start()
    for s in update(5, pl.ds(G - R3, R3), grid_v, aggb3, nodebase3, dec_v):
        s()
    put_grid[1].start()
    put_mesh.wait()
    for c in put_grid:
        c.wait()


def hand_on(grid, mesh, out_grid, out_mesh, grid_v, mesh_v, sem):
    pieces = [(grid, grid_v, out_grid), (mesh, mesh_v, out_mesh)]
    takes = [pltpu.make_async_copy(a, b, sem.at[n]) for n, (a, b, _) in enumerate(pieces)]
    gives = [pltpu.make_async_copy(b, c, sem.at[2 + n]) for n, (_, b, c) in enumerate(pieces)]
    for c in takes:
        c.start()
    for a, b in ((takes[1], gives[1]), (takes[0], gives[0])):
        a.wait()
        b.start()
    for c in gives:
        c.wait()


def per_device(*args):
    any_space = pl.BlockSpec(memory_space=pl.ANY)
    dma = pltpu.SemaphoreType.DMA
    regular = pltpu.SemaphoreType.REGULAR
    vm = pltpu.VMEM
    sm = pltpu.SMEM
    i32 = jnp.int32
    shapes = (jax.ShapeDtypeStruct((G, D), BF16), jax.ShapeDtypeStruct((M, D), BF16))
    results = pl.pallas_call(
        kernel,
        out_shape=shapes,
        in_specs=[any_space] * len(args),
        out_specs=(any_space, any_space),
        scratch_shapes=[
            vm((G, D), BF16), vm((M, D), BF16), vm((K, M), i32), vm((K, M), i32), vm((K3, G), i32),
            vm((6, 3, D, D), BF16), vm((6, 2, D), F32),
            vm((M, 128), i32), vm((M, 128), i32), vm((BLOCKS3 * 8, 128), i32),
            sm((M, 128), i32), sm((M, 128), i32), sm((BLOCKS3 * 8, 128), i32),
            vm((ROWS1 * 4 + 8, 128), F32), vm((ROWS2 * 4 + 8, 128), F32), vm((ROWS3 * 4 + 8, 128), F32),
            vm((M, D), F32), vm((M, D), F32), vm((G, D), F32), vm((G, D), F32),
            vm((E * 4, 128), F32), vm((E * 4, 128), F32),
            vm((E, D), BF16), vm((E, D), BF16), vm((E, D), F32), vm((E, D), F32),
            vm((M, D), BF16), vm((M, D), BF16), vm((M, D), BF16), vm((G, D), BF16), vm((G, D), BF16),
            vm((GB * 4, 128), BF16), vm((9, GB * 4, 128), BF16),
            vm((MB * 4, 128), BF16), vm((9, MB * 4, 128), BF16),
            vm((2, CHIPS, CM * 4, 128), BF16),
            vm((MB * 4, 128), BF16), vm((9, MB * 4, 128), BF16),
            dma((12,)), dma((7,)), dma((3,)), dma((3,)),
            dma((9, 2)), dma((9, 2)), dma((9,)), dma((9,)), dma((9,)), dma((9,)),
            dma, dma, dma, dma,
            regular, regular,
        ],
        compiler_params=pltpu.CompilerParams(
            collective_id=0, has_side_effects=True, vmem_limit_bytes=60 * 1024 * 1024
        ),
    )(*args)
    return pl.pallas_call(
        hand_on,
        out_shape=shapes,
        in_specs=[any_space] * 2,
        out_specs=(any_space, any_space),
        scratch_shapes=[vm((G, D), BF16), vm((M, D), BF16), dma((4,))],
        compiler_params=pltpu.CompilerParams(vmem_limit_bytes=60 * 1024 * 1024),
    )(*results)


def solution(mesh):
    assert dict(mesh.shape) == {"gx": NX, "gy": NY}
    split = P(("gx", "gy"), None)
    lists = P(None, ("gx", "gy"))
    return jax.shard_map(
        per_device,
        mesh=mesh,
        in_specs=(split, split, lists, lists, lists) + (P(),) * 12,
        out_specs=(split, split),
        check_vma=False,
    )
```
